128 devices in a mesh: gx: 4 (over z_lo, core), gy: 16 (over x, y), gz: 2 (over z_hi).
Axes of the slice: x: 4, y: 4, z: 4 (z_hi: 2, z_lo: 2; z = z_hi * 2 + z_lo), core: 2. Of those that a mesh axis runs over, the one named last changes fastest.
Arguments:
- eigvecs: bfloat16 [64, 128, 96, 512], P('gx', 'gy', 'gz'), may hold values from -7 to 7, as said below
- material: float32 [2, 64, 128, 96], P(None, 'gx', 'gy', 'gz'), may hold values from 0.5 to 2
Outputs:
- stiffness: float32 [512, 512], P(('gx', 'gy', 'gz'))
- mass_matrix: float32 [512, 512], P(('gx', 'gy', 'gz'))
The draws below stay inside these ranges and needn't reach their ends.
Inputs may be any that keep to these rules, and one draw needn't show every extreme that they name: `eigvecs`: entries are a rough part plus a part that varies slowly over the grid.
All inputs are finite; a program needn't handle non-finite values.
Results may differ from the reference program's by a relative error of at most 0.0003.
Values may be sent and summed in bfloat16 or wider, within the bound.
A program may use at most 128 MiB of HBM per device.

```python
import math
import jax
import jax.numpy as jnp
from jax import lax

K = 512
NX = 64
NY = 128
NZ = 96


def draw_eigvecs(key, part):
    keys = jax.random.split(key, 7)
    rough = jnp.clip(jax.random.normal(keys[0], (NX, NY, NZ, K), jnp.float32), -4.0, 4.0)
    amplitude = 2.0
    freq_x = jax.random.randint(keys[1], (K,), 1, 4).astype(jnp.float32)
    freq_y = jax.random.randint(keys[2], (K,), 1, 4).astype(jnp.float32)
    freq_z = jax.random.randint(keys[3], (K,), 1, 4).astype(jnp.float32)
    phase_x = jax.random.uniform(keys[4], (K,), jnp.float32)
    phase_y = jax.random.uniform(keys[5], (K,), jnp.float32)
    phase_z = jax.random.uniform(keys[6], (K,), jnp.float32)
    coord_x = jnp.arange(NX, dtype=jnp.float32)[:, None] / NX
    coord_y = jnp.arange(NY, dtype=jnp.float32)[:, None] / NY
    coord_z = jnp.arange(NZ, dtype=jnp.float32)[:, None] / NZ
    wave_x = jnp.cos(2.0 * jnp.pi * (coord_x * freq_x + phase_x))
    wave_y = jnp.cos(2.0 * jnp.pi * (coord_y * freq_y + phase_y))
    wave_z = jnp.cos(2.0 * jnp.pi * (coord_z * freq_z + phase_z))
    smooth = wave_x[:, None, None, :] * wave_y[None, :, None, :] * wave_z[None, None, :, :]
    return (rough + amplitude * smooth).astype(jnp.bfloat16)


def shard_levels(own_key, shape, cuts, low, top_value):
    factor_of = 1.0
    for dim, shards_of in cuts:
        heights = jax.random.uniform(jax.random.fold_in(jax.random.fold_in(own_key, 6), dim), (shards_of,), jnp.float32, low / len(cuts), top_value / len(cuts))
        factor_of = factor_of * jnp.repeat(jnp.exp(heights), shape[dim] // shards_of).reshape((-1,) + (1,) * (len(shape) - 1 - dim))
    return factor_of


def setup_inputs(seed: int = 0) -> dict:
    streams_of = jax.random.split(jax.random.key(seed), 3)
    eigvecs = draw_eigvecs(jax.random.fold_in(streams_of[2], 71), 0)
    material = jnp.clip(jnp.exp(math.log(2.0) - 1.3862944 * jax.random.uniform(streams_of[1], (2, NX, NY, NZ), jnp.float32) ** shard_levels(streams_of[1], (2, NX, NY, NZ), ((1, 4), (2, 16), (3, 2)), -0.2, 0.2)), 0.5, 2.0)
    return {"eigvecs": eigvecs, "material": material}


stencil_offsets = [(dx, dy, dz) for dx in (-1, 0, 1) for dy in (-1, 0, 1) for dz in (-1, 0, 1) if (dx, dy, dz) != (0, 0, 0)]


def coupling(offset):
    nonzero = sum(abs(entry) for entry in offset)
    return 0.25 * 0.5 ** (nonzero - 1)


def mass_weight(offset):
    weight = 1.0
    for entry in offset:
        weight = weight * (4.0 / 6.0 if entry == 0 else 1.0 / 6.0)
    return weight


def apply_operators(padded, padded_material):
    size_x = padded.shape[0] - 2
    size_y = padded.shape[1] - 2
    size_z = padded.shape[2] - 2
    centre = padded[1:-1, 1:-1, 1:-1].astype(jnp.float32)
    kappa_centre = padded_material[0, 1:-1, 1:-1, 1:-1]
    rho_centre = padded_material[1, 1:-1, 1:-1, 1:-1]
    stiff_sum = jnp.zeros(centre.shape, jnp.float32)
    mass_sum = mass_weight((0, 0, 0)) * rho_centre[..., None] * centre
    for offset in stencil_offsets:
        lower = (1 + offset[0], 1 + offset[1], 1 + offset[2])
        shifted = padded[lower[0]:lower[0] + size_x, lower[1]:lower[1] + size_y, lower[2]:lower[2] + size_z].astype(jnp.float32)
        kappa_side = padded_material[0, lower[0]:lower[0] + size_x, lower[1]:lower[1] + size_y, lower[2]:lower[2] + size_z]
        rho_side = padded_material[1, lower[0]:lower[0] + size_x, lower[1]:lower[1] + size_y, lower[2]:lower[2] + size_z]
        stiff_sum = stiff_sum + (coupling(offset) * 0.5 * (kappa_centre + kappa_side))[..., None] * (centre - shifted)
        mass_sum = mass_sum + (mass_weight(offset) * 0.5 * (rho_centre + rho_side))[..., None] * shifted
    return stiff_sum.astype(jnp.bfloat16), mass_sum.astype(jnp.bfloat16)


def reference(eigvecs, material):
    cells = NX * NY * NZ
    block_cols = 32
    padded_material = jnp.pad(material, ((0, 0), (1, 1), (1, 1), (1, 1)))
    flat_vectors = eigvecs.reshape(cells, K)

    def column_block(block_index):
        first_col = block_index * block_cols
        col_block = lax.dynamic_slice_in_dim(eigvecs, first_col, block_cols, 3)
        padded = jnp.pad(col_block, ((1, 1), (1, 1), (1, 1), (0, 0)))
        stiff_vecs, mass_vecs = apply_operators(padded, padded_material)
        dims = (((0,), (0,)), ((), ()))
        stiff_cols = lax.dot_general(flat_vectors, stiff_vecs.reshape(cells, block_cols), dims, preferred_element_type=jnp.float32)
        mass_cols = lax.dot_general(flat_vectors, mass_vecs.reshape(cells, block_cols), dims, preferred_element_type=jnp.float32)
        return stiff_cols, mass_cols

    stiff_blocks, mass_blocks = lax.map(column_block, jnp.arange(K // block_cols, dtype=jnp.int32))
    stiffness = jnp.transpose(stiff_blocks, (1, 0, 2)).reshape(K, K) / cells
    mass_matrix = jnp.transpose(mass_blocks, (1, 0, 2)).reshape(K, K) / cells
    return stiffness, mass_matrix
```

```python
import jax
import jax.numpy as jnp
import numpy as np
from jax import lax
from jax.experimental import pallas as pl
from jax.experimental.pallas import tpu as pltpu
from jax.sharding import PartitionSpec as P

MESH = pl.DeviceIdType.MESH
F32, BF16 = jnp.float32, jnp.bfloat16
PC, PM = 1.0 / 16.0, 1.0 / 216.0


def taps(rows, cols, middle):
    gap = np.abs(rows[:, None] - cols[None, :])
    return np.where(gap == 0, middle, np.where(gap == 1, 1, 0))


def pair_weights(halo, own, middle):
    total = 1
    for h, o in zip(halo, own):
        total = total * taps(h, o, middle)
    return total


def grid(*axes):
    return [a.reshape(-1) for a in np.meshgrid(*axes, indexing="ij")]


def stacked(halo, own, pad):
    w = np.concatenate([pair_weights(halo, own, 2), pair_weights(halo, own, 4)], axis=1)
    w = np.concatenate([w, np.zeros((pad, w.shape[1]), w.dtype)], axis=0)
    return w.astype(np.float32)


def weight_arrays(nx, ny, nz):
    hx = nx // 2
    y, z = grid(np.arange(ny), np.arange(nz))
    plane = stacked([y, z], [y, z], 0)
    hxx, hzz = grid(np.arange(-1, hx + 1), np.arange(nz))
    oxx, ozz = grid(np.arange(hx), np.arange(nz))
    wy = stacked(
        [hxx, hzz, 0 * hxx + 1], [oxx, ozz, 0 * oxx], (-hxx.size) % 128
    )
    wx = stacked([y, z, 0 * y + 1], [y, z, 0 * y], 0)
    far = 99
    slabs = []
    xs = np.arange(nx)
    for yy in range(ny):
        slabs.append((xs, 0 * xs + yy))
    ys = np.concatenate([np.arange(ny), far + 0 * np.arange(nx - ny)])
    first = np.where(xs == 0, 0, far)
    last = np.where(xs == nx - 1, 0, far)
    slabs += [(xs, 0 * xs - 1), (xs, 0 * xs + ny)]
    slabs += [(0 * xs - 1, ys), (0 * xs + nx, ys)]
    slabs += [(last - 1, 0 * xs - 1), (last - 1, 0 * xs + ny)]
    slabs += [(first + nx, 0 * xs - 1), (first + nx, 0 * xs + ny)]
    zx = np.concatenate([s[0] for s in slabs])
    zy = np.concatenate([s[1] for s in slabs])
    oyy, oxx = grid(np.arange(ny), np.arange(nx))
    wz = stacked([zx, zy, 0 * zx + 1], [oxx, oyy, 0 * oxx], 0)
    return plane, wy, wx, wz


def nt(a, b):
    return lax.dot_general(a, b, (((1,), (1,)), ((), ())), preferred_element_type=F32)


def nn(a, b):
    return jnp.dot(a, b, preferred_element_type=F32)


def exact(a, b):
    return jnp.dot(a, b, preferred_element_type=F32, precision=lax.Precision.HIGHEST)


def exact_nt(a, b):
    return lax.dot_general(
        a, b, (((1,), (1,)), ((), ())), preferred_element_type=F32,
        precision=lax.Precision.HIGHEST,
    )


def local_kernel(
    dims, scale,
    v_ref, mat_ref, faces_ref, zf_ref, zx_ref, wp_ref, wy_ref, wx_ref, wz_ref,
    out_ref,
    vbuf, vt, fbuf, ym, acc, hy, hx, hz, fh, vsem, send_sem, recv_sem,
):
    nx, ny, nz, cols, ngx, ngy = dims
    n = ny * nz
    gx, gy, gz = lax.axis_index("gx"), lax.axis_index("gy"), lax.axis_index("gz")
    hx_n = nx // 2

    loads = [pltpu.make_async_copy(v_ref.at[x], vbuf.at[x], vsem.at[x]) for x in range(nx)]
    for load in loads:
        load.start()

    def zrow(k):
        return hz.at[k]

    links = [
        ((0, 1), False, v_ref.at[:, ny - 1], hy.at[pl.ds(1, nx)]),
        ((1, 1), False, v_ref.at[nx - 1, ny - 1], hy.at[0]),
        ((-1, 1), False, v_ref.at[0, ny - 1], hy.at[nx + 1]),
        ((1, 0), False, v_ref.at[nx - 1], hx),
        ((0, 0), True, zf_ref, hz.at[pl.ds(0, ny)]),
        ((0, 1), True, zf_ref.at[ny - 1], zrow(ny)),
        ((0, -1), True, zf_ref.at[0], zrow(ny + 1)),
        ((1, 0), True, zx_ref.at[1], zrow(ny + 2)),
        ((-1, 0), True, zx_ref.at[0], zrow(ny + 3)),
        ((1, 1), True, zf_ref.at[ny - 1], zrow(ny + 4)),
        ((1, -1), True, zf_ref.at[0], zrow(ny + 5)),
        ((-1, 1), True, zf_ref.at[ny - 1], zrow(ny + 6)),
        ((-1, -1), True, zf_ref.at[0], zrow(ny + 7)),
    ]

    def inside(dx, dy):
        ok = None
        for move, at, count in ((dx, gx, ngx), (dy, gy, ngy)):
            here = None
            if move == 1:
                here = at < count - 1
            if move == -1:
                here = at > 0
            if here is not None:
                ok = here if ok is None else jnp.logical_and(ok, here)
        return ok

    def both(a, b):
        return b if a is None else jnp.logical_and(a, b)

    def sends_if(link):
        (dx, dy), cut, _, _ = link
        ok = inside(dx, dy)
        return both(ok, gz == 0) if cut else ok

    def gets_if(link):
        (dx, dy), cut, _, _ = link
        ok = inside(-dx, -dy)
        return both(ok, gz == 1) if cut else ok

    hy[...] = jnp.zeros_like(hy)
    hx[...] = jnp.zeros_like(hx)
    hz[...] = jnp.zeros_like(hz)
    fh[...] = jnp.zeros_like(fh)

    barrier = pltpu.get_barrier_semaphore()
    targets = 0
    for link in links:
        (dx, dy), cut, _, _ = link
        source = (gx - dx, gy - dy, 0 if cut else gz)

        @pl.when(gets_if(link))
        def _(source=source):
            pl.semaphore_signal(barrier, inc=1, device_id=source, device_id_type=MESH)

        targets = targets + sends_if(link).astype(jnp.int32)

    @pl.when(targets > 0)
    def _():
        pl.semaphore_wait(barrier, targets)

    copies = []
    for k, link in enumerate(links):
        (dx, dy), cut, source, target = link
        device = (gx + dx, gy + dy, 1 if cut else gz)
        pair = [
            pltpu.make_async_remote_copy(
                src_ref=s, dst_ref=t, send_sem=send_sem.at[2 * k + j],
                recv_sem=recv_sem.at[2 * k + j], device_id=device, device_id_type=MESH,
            )
            for j, (s, t) in enumerate(((faces_ref, fh.at[k]), (source, target)))
        ]
        copies.append(pair)

        @pl.when(sends_if(link))
        def _(pair=pair):
            for copy in pair:
                copy.start()

    kappa, rho = mat_ref[0], mat_ref[1]
    filtered = exact(kappa, wp_ref[:, :n].astype(F32))
    zero = jnp.zeros((1, n), F32)
    around = (
        jnp.concatenate([zero, filtered[:-1]], axis=0)
        + 2.0 * filtered
        + jnp.concatenate([filtered[1:], zero], axis=0)
    )
    diag = 0.5 * (3.5 * kappa + PC * around - 0.5 * kappa)
    coef_v = diag + 0.5 * kappa
    coef_s = PC * kappa
    coef_m = PM * rho

    def stage_a(x):
        if x >= nx:
            return
        loads[x].wait()
        t = vbuf[x].reshape(n, cols).T
        vt[x // 2, :, (x % 2) * n : (x % 2 + 1) * n] = t
        fbuf[x % 6] = nn(t, wp_ref[...])

    chunk = 64

    def stage_b(x):
        half = (x % 2) * n
        buf = (x // 2) % 2
        cv, cs, cm = (c[x : x + 1, :] for c in (coef_v, coef_s, coef_m))
        for r in range(0, cols, chunk):
            rows = slice(r, r + chunk)
            mid_s = fbuf[x % 6, rows, :n]
            mid_m = fbuf[x % 6, rows, n:]
            s, m = 2.0 * mid_s, 4.0 * mid_m
            for near in (x - 1, x + 1):
                if 0 <= near < nx:
                    s = s + fbuf[near % 6, rows, :n]
                    m = m + fbuf[near % 6, rows, n:]
            v = vt[x // 2, rows, half : half + n].astype(F32)
            ym[buf, rows, half : half + n] = (cv * v - cs * s).astype(BF16)
            ym[buf, cols + r : cols + r + chunk, half : half + n] = (cm * m).astype(BF16)

    def stage_c(pair):
        for h in range(2):
            part = nt(vt[pair], ym[pair % 2, h * cols : (h + 1) * cols])
            if pair == 0:
                acc[h] = part
            else:
                acc[h] += part

    pairs = nx // 2
    for x in range(3):
        stage_a(x)
    for i in range(pairs):
        stage_a(2 * i + 3)
        stage_a(2 * i + 4)
        stage_b(2 * i)
        stage_b(2 * i + 1)
        if i > 0:
            stage_c(i - 1)
    stage_c(pairs - 1)

    for k, link in enumerate(links):
        @pl.when(gets_if(link))
        def _(k=k):
            for copy in copies[k]:
                copy.wait_recv()

    def group(halo, kh, rh, own, ko, ro, w_ref):
        m = own.shape[1]
        wc, wm = w_ref[:, :m], w_ref[:, m:]
        ht = halo.T
        plain = nn(ht, w_ref[...])
        h32 = ht.astype(F32)
        by_kappa = nn((h32 * kh).astype(BF16), wc)
        by_rho = nn((h32 * rh).astype(BF16), wm)
        wc32 = wc.astype(F32)
        own_diag = (0.5 * PC) * exact(jnp.broadcast_to(kh, (8, kh.shape[1])), wc32)[:1]
        far_diag = (0.5 * PC) * exact_nt(jnp.broadcast_to(ko, (8, m)), wc32)[:1]
        us = own_diag * own.astype(F32) - PC * (ko * plain[:, :m] + by_kappa)
        um = PM * (ro * plain[:, m:] + by_rho)
        acc[0] += nt(own, us.astype(BF16)) + nt(ht, (far_diag * h32).astype(BF16))
        acc[1] += nt(own, um.astype(BF16))

    def row(k, r, lo, hi):
        return fh[k, r : r + 1, lo:hi]

    def wide(x):
        return jnp.concatenate(x, axis=1)

    kp = wy_ref.shape[0]
    used = (hx_n + 2) * nz
    blank = jnp.zeros((1, kp - used), F32)
    edge = (nx - 1) * nz
    for side in range(2):
        if side == 0:
            pick = lambda r: wide([row(1, r, edge, edge + nz), row(0, r, 0, used - nz), blank])
        else:
            pick = lambda r: wide(
                [row(0, r, (hx_n - 1) * nz, nx * nz), row(2, r, 0, nz), blank]
            )
        slots = -(-kp // nz)
        start = side * hx_n
        halo = hy[start : start + slots].reshape(slots * nz, cols)[:kp]
        own = vbuf[start : start + hx_n, 0].reshape(hx_n * nz, cols).T
        mine = [
            wide([mat_ref[j, x : x + 1, :nz] for x in range(start, start + hx_n)])
            for j in range(2)
        ]
        group(halo, pick(0), pick(1), own, mine[0], mine[1], wy_ref)

    group(
        hx[...].reshape(n, cols), row(3, 2, 0, n), row(3, 3, 0, n),
        vt[0, :, :n], kappa[:1], rho[:1], wx_ref,
    )

    nf = nx * ny
    low, high = (nf - nx, nf), (0, nx)

    def zpick(r):
        spans = [(4, (0, nf)), (5, low), (6, high), (7, (nf + nx, nf + 2 * nx)),
                 (8, (nf, nf + nx)), (9, low), (10, high), (11, low), (12, high)]
        return wide([row(k, r, lo, hi) for k, (lo, hi) in spans])

    group(
        hz[...].reshape((ny + 8) * nx, cols), zpick(4), zpick(5),
        zf_ref[...].reshape(nf, cols).T, faces_ref[4:5, :nf], faces_ref[5:6, :nf], wz_ref,
    )

    for h in range(2):
        total = acc[h]
        out_ref[:, h * cols : (h + 1) * cols] = (total + total.T) * scale

    for k, link in enumerate(links):
        @pl.when(sends_if(link))
        def _(k=k):
            for copy in copies[k]:
                copy.wait_send()


def local_sums(eigvecs, material):
    nx, ny, nz, cols = eigvecs.shape
    n = ny * nz
    count = {a: lax.axis_size(a) for a in ("gx", "gy", "gz")}
    cells = nx * ny * nz * count["gx"] * count["gy"] * count["gz"]
    plane, wy, wx, wz = (jnp.asarray(w, BF16) for w in weight_arrays(nx, ny, nz))
    at = jnp.where(lax.axis_index("gz") == 0, nz - 1, 0)
    zface = lax.dynamic_index_in_dim(eigvecs, at, 2, False)
    zf = jnp.swapaxes(zface, 0, 1)
    zx = jnp.pad(zface[:: nx - 1], ((0, 0), (0, nx - ny), (0, 0)))
    mz = lax.dynamic_index_in_dim(material, at, 3, False)
    flat = material.reshape(2, nx, n)
    width = nx * nz

    def fit(a):
        a = a.reshape(2, -1)
        return jnp.pad(a, ((0, 0), (0, width - a.shape[1])))

    mzx = jnp.pad(mz[:, :: nx - 1], ((0, 0), (0, 0), (0, nx - ny)))
    faces = jnp.concatenate(
        [
            fit(material[:, :, ny - 1]),
            fit(material[:, nx - 1]),
            fit(jnp.concatenate([jnp.swapaxes(mz, 1, 2).reshape(2, -1), mzx.reshape(2, -1)], 1)),
            jnp.zeros((2, width), F32),
        ],
        axis=0,
    )
    anyspace = pl.BlockSpec(memory_space=pl.ANY)
    vmem = pl.BlockSpec(memory_space=pltpu.VMEM)
    kernel = lambda *refs: local_kernel(
        (nx, ny, nz, cols, count["gx"], count["gy"]), 0.5 / cells, *refs
    )
    return pl.pallas_call(
        kernel,
        out_shape=jax.ShapeDtypeStruct((cols, 2 * cols), F32),
        in_specs=[anyspace] + [vmem] * 8,
        out_specs=vmem,
        scratch_shapes=[
            pltpu.VMEM((nx, ny, nz, cols), BF16),
            pltpu.VMEM((nx // 2, cols, 2 * n), BF16),
            pltpu.VMEM((6, cols, 2 * n), F32),
            pltpu.VMEM((2, 2 * cols, 2 * n), BF16),
            pltpu.VMEM((2, cols, cols), F32),
            pltpu.VMEM((nx + 3, nz, cols), BF16),
            pltpu.VMEM((ny, nz, cols), BF16),
            pltpu.VMEM((ny + 8, nx, cols), BF16),
            pltpu.VMEM((13, 8, width), F32),
            pltpu.SemaphoreType.DMA((nx,)),
            pltpu.SemaphoreType.DMA((26,)),
            pltpu.SemaphoreType.DMA((26,)),
        ],
        compiler_params=pltpu.CompilerParams(
            collective_id=0, has_side_effects=True, vmem_limit_bytes=63 * 1024 * 1024
        ),
        name="local_sums",
    )(eigvecs, flat, faces, zf, zx, plane, wy, wx, wz)


def split_up(x, dim, devices):
    dims = x.shape
    parts = x.reshape(*dims[:dim], devices, dims[dim] // devices, *dims[dim + 1 :])
    return jnp.moveaxis(parts, dim, 0)


def sum_at_owner(x, axis, dim):
    devices = lax.axis_size(axis)
    parts = lax.all_to_all(split_up(x, dim, devices), axis, 0, 0, tiled=True)
    return jnp.sum(parts, axis=0)


def per_device(eigvecs, material):
    columns = eigvecs.shape[3]
    part = local_sums(eigvecs, material)
    summed = sum_at_owner(sum_at_owner(sum_at_owner(part, "gx", 0), "gy", 0), "gz", 0)
    return summed[:, :columns], summed[:, columns:]


def solution(mesh):
    return jax.shard_map(
        per_device,
        mesh=mesh,
        in_specs=(P("gx", "gy", "gz", None), P(None, "gx", "gy", "gz")),
        out_specs=(P(("gx", "gy", "gz"), None), P(("gx", "gy", "gz"), None)),
        check_vma=False,
    )
```

```python
import jax
import jax.numpy as jnp
import numpy as np
from jax import lax
from jax.experimental import pallas as pl
from jax.experimental.pallas import tpu as pltpu
from jax.sharding import PartitionSpec as P

MESH = pl.DeviceIdType.MESH
F32, BF16 = jnp.float32, jnp.bfloat16
PC, PM = 1.0 / 16.0, 1.0 / 216.0


def taps(rows, cols, middle):
    gap = np.abs(rows[:, None] - cols[None, :])
    return np.where(gap == 0, middle, np.where(gap == 1, 1, 0))


def pair_weights(halo, own, middle):
    total = 1
    for h, o in zip(halo, own):
        total = total * taps(h, o, middle)
    return total


def grid(*axes):
    return [a.reshape(-1) for a in np.meshgrid(*axes, indexing="ij")]


def stacked(halo, own, pad):
    w = np.concatenate([pair_weights(halo, own, 2), pair_weights(halo, own, 4)], axis=1)
    w = np.concatenate([w, np.zeros((pad, w.shape[1]), w.dtype)], axis=0)
    return w.astype(np.float32)


def weight_arrays(nx, ny, nz):
    hx = nx // 2
    y, z = grid(np.arange(ny), np.arange(nz))
    plane = stacked([y, z], [y, z], 0)
    hxx, hzz = grid(np.arange(-1, hx + 1), np.arange(nz))
    oxx, ozz = grid(np.arange(hx), np.arange(nz))
    wy = stacked(
        [hxx, hzz, 0 * hxx + 1], [oxx, ozz, 0 * oxx], (-hxx.size) % 128
    )
    wx = stacked([y, z, 0 * y + 1], [y, z, 0 * y], 0)
    far = 99
    slabs = []
    xs = np.arange(nx)
    for yy in range(ny):
        slabs.append((xs, 0 * xs + yy))
    ys = np.concatenate([np.arange(ny), far + 0 * np.arange(nx - ny)])
    first = np.where(xs == 0, 0, far)
    last = np.where(xs == nx - 1, 0, far)
    slabs += [(xs, 0 * xs - 1), (xs, 0 * xs + ny)]
    slabs += [(0 * xs - 1, ys), (0 * xs + nx, ys)]
    slabs += [(last - 1, 0 * xs - 1), (last - 1, 0 * xs + ny)]
    slabs += [(first + nx, 0 * xs - 1), (first + nx, 0 * xs + ny)]
    zx = np.concatenate([s[0] for s in slabs])
    zy = np.concatenate([s[1] for s in slabs])
    oyy, oxx = grid(np.arange(ny), np.arange(nx))
    wz = stacked([zx, zy, 0 * zx + 1], [oxx, oyy, 0 * oxx], 0)
    return plane, wy, wx, wz


def nt(a, b):
    return lax.dot_general(a, b, (((1,), (1,)), ((), ())), preferred_element_type=F32)


def nn(a, b):
    return jnp.dot(a, b, preferred_element_type=F32)


def exact(a, b):
    return jnp.dot(a, b, preferred_element_type=F32, precision=lax.Precision.HIGHEST)


def exact_nt(a, b):
    return lax.dot_general(
        a, b, (((1,), (1,)), ((), ())), preferred_element_type=F32,
        precision=lax.Precision.HIGHEST,
    )


ORDERS = ("yxz", "xzy", "zyx", "xyz")
GONE = {"x": "x", "y": "y", "z": "lh"}
SIZE = {"l": 2, "h": 2, "x": 4, "y": 4}
tiles = len(ORDERS)


def exchange_start(t, s, held, pick, place, device_of, send, stage):
    buf, dims = held
    dim = ORDERS[t][s]
    copies = []
    for j in range(3):
        at = lax.rem(place[dim] + j + 1, 4)
        copies.append(
            send(
                buf.at[pick(buf, dims, dim, at)], stage[s + 1][t].at[j],
                tiles + (s * tiles + t) * 3 + j, device_of(dim, at),
            )
        )
    return copies


def partners(gx, gy, gz):
    core, z = lax.rem(gx, 2), gz * 2 + gx // 2
    x, y = gy // 4, lax.rem(gy, 4)
    found = [(gx + 1 - 2 * core, gy, gz)]
    for j in range(1, 4):
        found.append((gx, x * 4 + lax.rem(y + j, 4), gz))
        found.append((gx, lax.rem(x + j, 4) * 4 + y, gz))
        zz = lax.rem(z + j, 4)
        found.append((lax.rem(zz, 2) * 2 + core, gy, zz // 2))
    return found


def stage_shapes():
    shapes, keeps = [[(2, 4, 4, 2, 8, 128)] * tiles], []
    for s in range(3):
        row, kept = [], []
        for t in range(tiles):
            gone = "".join(GONE[d] for d in ORDERS[t][: s + 1])
            left = tuple(SIZE[d] for d in "lxyh" if d not in gone) + (8, 128)
            row.append((3,) + left)
            kept.append(left)
        shapes.append(row)
        keeps.append(kept)
    return shapes, keeps[:2]


def local_kernel(
    dims, scale,
    v_ref, mat_ref, faces_ref, zf_ref, zx_ref, wp_ref, wy_ref, wx_ref, wz_ref,
    stiff_ref, mass_ref,
    vbuf, vt, fbuf, ym, acc, hy, hx, hz, fh, vsem, send_sem, recv_sem,
    q, rsend, rrecv, *rest,
):
    stage = [rest[s * tiles : (s + 1) * tiles] for s in range(4)]
    keep = [rest[(4 + s) * tiles : (5 + s) * tiles] for s in range(2)]
    nx, ny, nz, cols, ngx, ngy = dims
    n = ny * nz
    gx, gy, gz = lax.axis_index("gx"), lax.axis_index("gy"), lax.axis_index("gz")
    hx_n = nx // 2

    loads = [pltpu.make_async_copy(v_ref.at[x], vbuf.at[x], vsem.at[x]) for x in range(nx)]
    for load in loads:
        load.start()

    def zrow(k):
        return hz.at[k]

    links = [
        ((0, 1), False, v_ref.at[:, ny - 1], hy.at[pl.ds(1, nx)]),
        ((1, 1), False, v_ref.at[nx - 1, ny - 1], hy.at[0]),
        ((-1, 1), False, v_ref.at[0, ny - 1], hy.at[nx + 1]),
        ((1, 0), False, v_ref.at[nx - 1], hx),
        ((0, 0), True, zf_ref, hz.at[pl.ds(0, ny)]),
        ((0, 1), True, zf_ref.at[ny - 1], zrow(ny)),
        ((0, -1), True, zf_ref.at[0], zrow(ny + 1)),
        ((1, 0), True, zx_ref.at[1], zrow(ny + 2)),
        ((-1, 0), True, zx_ref.at[0], zrow(ny + 3)),
        ((1, 1), True, zf_ref.at[ny - 1], zrow(ny + 4)),
        ((1, -1), True, zf_ref.at[0], zrow(ny + 5)),
        ((-1, 1), True, zf_ref.at[ny - 1], zrow(ny + 6)),
        ((-1, -1), True, zf_ref.at[0], zrow(ny + 7)),
    ]

    def inside(dx, dy):
        ok = None
        for move, at, count in ((dx, gx, ngx), (dy, gy, ngy)):
            here = None
            if move == 1:
                here = at < count - 1
            if move == -1:
                here = at > 0
            if here is not None:
                ok = here if ok is None else jnp.logical_and(ok, here)
        return ok

    def both(a, b):
        return b if a is None else jnp.logical_and(a, b)

    def sends_if(link):
        (dx, dy), cut, _, _ = link
        ok = inside(dx, dy)
        return both(ok, gz == 0) if cut else ok

    def gets_if(link):
        (dx, dy), cut, _, _ = link
        ok = inside(-dx, -dy)
        return both(ok, gz == 1) if cut else ok

    hy[...] = jnp.zeros_like(hy)
    hx[...] = jnp.zeros_like(hx)
    hz[...] = jnp.zeros_like(hz)
    fh[...] = jnp.zeros_like(fh)

    barrier = pltpu.get_barrier_semaphore()
    targets = 0
    for link in links:
        (dx, dy), cut, _, _ = link
        source = (gx - dx, gy - dy, 0 if cut else gz)

        @pl.when(gets_if(link))
        def _(source=source):
            pl.semaphore_signal(barrier, inc=1, device_id=source, device_id_type=MESH)

        targets = targets + sends_if(link).astype(jnp.int32)
    for device in partners(gx, gy, gz):
        pl.semaphore_signal(barrier, inc=1, device_id=device, device_id_type=MESH)
    pl.semaphore_wait(barrier, targets + 10)

    copies = []
    for k, link in enumerate(links):
        (dx, dy), cut, source, target = link
        device = (gx + dx, gy + dy, 1 if cut else gz)
        pair = [
            pltpu.make_async_remote_copy(
                src_ref=s, dst_ref=t, send_sem=send_sem.at[2 * k + j],
                recv_sem=recv_sem.at[2 * k + j], device_id=device, device_id_type=MESH,
            )
            for j, (s, t) in enumerate(((faces_ref, fh.at[k]), (source, target)))
        ]
        copies.append(pair)

        @pl.when(sends_if(link))
        def _(pair=pair):
            for copy in pair:
                copy.start()

    kappa, rho = mat_ref[0], mat_ref[1]
    filtered = exact(kappa, wp_ref[:, :n].astype(F32))
    zero = jnp.zeros((1, n), F32)
    around = (
        jnp.concatenate([zero, filtered[:-1]], axis=0)
        + 2.0 * filtered
        + jnp.concatenate([filtered[1:], zero], axis=0)
    )
    diag = 0.5 * (3.5 * kappa + PC * around - 0.5 * kappa)
    coef_v = diag + 0.5 * kappa
    coef_s = PC * kappa
    coef_m = PM * rho

    def stage_a(x):
        if x >= nx:
            return
        loads[x].wait()
        t = vbuf[x].reshape(n, cols).T
        vt[x // 2, :, (x % 2) * n : (x % 2 + 1) * n] = t
        fbuf[x % 6] = nn(t, wp_ref[...])

    chunk = 64

    def stage_b(x):
        half = (x % 2) * n
        buf = (x // 2) % 2
        cv, cs, cm = (c[x : x + 1, :] for c in (coef_v, coef_s, coef_m))
        for r in range(0, cols, chunk):
            rows = slice(r, r + chunk)
            mid_s = fbuf[x % 6, rows, :n]
            mid_m = fbuf[x % 6, rows, n:]
            s, m = 2.0 * mid_s, 4.0 * mid_m
            for near in (x - 1, x + 1):
                if 0 <= near < nx:
                    s = s + fbuf[near % 6, rows, :n]
                    m = m + fbuf[near % 6, rows, n:]
            v = vt[x // 2, rows, half : half + n].astype(F32)
            ym[buf, rows, half : half + n] = (cv * v - cs * s).astype(BF16)
            ym[buf, cols + r : cols + r + chunk, half : half + n] = (cm * m).astype(BF16)

    def stage_c(pair):
        for h in range(2):
            part = nt(vt[pair], ym[pair % 2, h * cols : (h + 1) * cols])
            if pair == 0:
                acc[h] = part
            else:
                acc[h] += part

    pairs = nx // 2
    for x in range(3):
        stage_a(x)
    for i in range(pairs):
        stage_a(2 * i + 3)
        stage_a(2 * i + 4)
        stage_b(2 * i)
        stage_b(2 * i + 1)
        if i > 0:
            stage_c(i - 1)
    stage_c(pairs - 1)

    for k, link in enumerate(links):
        @pl.when(gets_if(link))
        def _(k=k):
            for copy in copies[k]:
                copy.wait_recv()

    def group(halo, kh, rh, own, ko, ro, w_ref):
        m = own.shape[1]
        wc, wm = w_ref[:, :m], w_ref[:, m:]
        ht = halo.T
        plain = nn(ht, w_ref[...])
        h32 = ht.astype(F32)
        by_kappa = nn((h32 * kh).astype(BF16), wc)
        by_rho = nn((h32 * rh).astype(BF16), wm)
        wc32 = wc.astype(F32)
        own_diag = (0.5 * PC) * exact(jnp.broadcast_to(kh, (8, kh.shape[1])), wc32)[:1]
        far_diag = (0.5 * PC) * exact_nt(jnp.broadcast_to(ko, (8, m)), wc32)[:1]
        us = own_diag * own.astype(F32) - PC * (ko * plain[:, :m] + by_kappa)
        um = PM * (ro * plain[:, m:] + by_rho)
        acc[0] += nt(own, us.astype(BF16)) + nt(ht, (far_diag * h32).astype(BF16))
        acc[1] += nt(own, um.astype(BF16))

    def row(k, r, lo, hi):
        return fh[k, r : r + 1, lo:hi]

    def wide(x):
        return jnp.concatenate(x, axis=1)

    kp = wy_ref.shape[0]
    used = (hx_n + 2) * nz
    blank = jnp.zeros((1, kp - used), F32)
    edge = (nx - 1) * nz
    for side in range(2):
        if side == 0:
            pick = lambda r: wide([row(1, r, edge, edge + nz), row(0, r, 0, used - nz), blank])
        else:
            pick = lambda r: wide(
                [row(0, r, (hx_n - 1) * nz, nx * nz), row(2, r, 0, nz), blank]
            )
        slots = -(-kp // nz)
        start = side * hx_n
        halo = hy[start : start + slots].reshape(slots * nz, cols)[:kp]
        own = vbuf[start : start + hx_n, 0].reshape(hx_n * nz, cols).T
        mine = [
            wide([mat_ref[j, x : x + 1, :nz] for x in range(start, start + hx_n)])
            for j in range(2)
        ]
        group(halo, pick(0), pick(1), own, mine[0], mine[1], wy_ref)

    group(
        hx[...].reshape(n, cols), row(3, 2, 0, n), row(3, 3, 0, n),
        vt[0, :, :n], kappa[:1], rho[:1], wx_ref,
    )

    nf = nx * ny
    low, high = (nf - nx, nf), (0, nx)

    def zpick(r):
        spans = [(4, (0, nf)), (5, low), (6, high), (7, (nf + nx, nf + 2 * nx)),
                 (8, (nf, nf + nx)), (9, low), (10, high), (11, low), (12, high)]
        return wide([row(k, r, lo, hi) for k, (lo, hi) in spans])

    group(
        hz[...].reshape((ny + 8) * nx, cols), zpick(4), zpick(5),
        zf_ref[...].reshape(nf, cols).T, faces_ref[4:5, :nf], faces_ref[5:6, :nf], wz_ref,
    )

    sums = []
    for h in range(2):
        total = acc[h]
        sums.append(((total + total.T) * scale).reshape(ngx * ngy, 8, cols))
    low_rows = lax.broadcasted_iota(jnp.int32, (ngx * ngy, 8, cols), 1) < 4
    turned = [pltpu.roll(part, 4, 1) for part in sums]
    shape = (2, 4, 4, 8, cols)
    core, zl = lax.rem(gx, 2), gx // 2
    first = jnp.where(low_rows, sums[0], turned[1]).reshape((2,) + shape)
    second = jnp.where(low_rows, turned[0], sums[1]).reshape((2,) + shape)
    for c in range(2):
        q[:, c, :, :, 0] = first[:, c]
        q[:, c, :, :, 1] = second[:, c]
    place = {"x": gy // 4, "y": lax.rem(gy, 4), "z": gz * 2 + zl}

    def device_of(dim, at):
        x, y, z = (at if dim == d else place[d] for d in "xyz")
        return (lax.rem(z, 2) * 2 + core, x * 4 + y, z // 2)

    pending = []

    def send(source, target, sem, device):
        copy = pltpu.make_async_remote_copy(
            src_ref=source, dst_ref=target, send_sem=rsend.at[sem], recv_sem=rrecv.at[sem],
            device_id=device, device_id_type=MESH,
        )
        copy.start()
        pending.append(copy)
        return copy

    def pick(buf, dims, dim, at):
        index = []
        for d in dims:
            hit = {"l": lax.rem(at, 2), "h": at // 2}.get(d) if dim == "z" else at if d == dim else None
            index.append(slice(None) if hit is None else hit)
        return tuple(index)

    swaps = []
    for t in range(tiles):
        lanes = slice(t * 128, (t + 1) * 128)
        swaps.append(
            send(
                q.at[:, 1 - core, :, :, :, :, lanes], stage[0][t], t,
                (zl * 2 + 1 - core, gy, gz),
            )
        )
    held = []
    for t in range(tiles):
        lanes = slice(t * 128, (t + 1) * 128)
        swaps[t].wait_recv()
        stage[0][t][...] += q[:, core, :, :, :, :, lanes]
        held.append((stage[0][t], "lxyh"))
        held[t] = (held[t], exchange_start(t, 0, held[t], pick, place, device_of, send, stage))
    for s in range(3):
        for t in range(tiles):
            (buf, dims), copies_t = held[t]
            dim = ORDERS[t][s]
            total = buf[pick(buf, dims, dim, place[dim])]
            for j, copy in enumerate(copies_t):
                copy.wait_recv()
                total = total + stage[s + 1][t][j]
            if s == 2:
                stiff_ref[:, t * 128 : (t + 1) * 128] = total[:4]
                mass_ref[:, t * 128 : (t + 1) * 128] = total[4:]
                continue
            left = "".join(d for d in dims if d not in GONE[dim])
            kept = keep[s][t]
            kept[...] = total
            held[t] = ((kept, left), None)
            held[t] = (held[t][0], exchange_start(t, s + 1, held[t][0], pick, place, device_of, send, stage))
    for copy in pending:
        copy.wait_send()
    for k, link in enumerate(links):
        @pl.when(sends_if(link))
        def _(k=k):
            for copy in copies[k]:
                copy.wait_send()


def local_sums(eigvecs, material):
    nx, ny, nz, cols = eigvecs.shape
    n = ny * nz
    count = {a: lax.axis_size(a) for a in ("gx", "gy", "gz")}
    cells = nx * ny * nz * count["gx"] * count["gy"] * count["gz"]
    plane, wy, wx, wz = (jnp.asarray(w, BF16) for w in weight_arrays(nx, ny, nz))
    at = jnp.where(lax.axis_index("gz") == 0, nz - 1, 0)
    zface = lax.dynamic_index_in_dim(eigvecs, at, 2, False)
    zf = jnp.swapaxes(zface, 0, 1)
    zx = jnp.pad(zface[:: nx - 1], ((0, 0), (0, nx - ny), (0, 0)))
    mz = lax.dynamic_index_in_dim(material, at, 3, False)
    flat = material.reshape(2, nx, n)
    width = nx * nz

    def fit(a):
        a = a.reshape(2, -1)
        return jnp.pad(a, ((0, 0), (0, width - a.shape[1])))

    mzx = jnp.pad(mz[:, :: nx - 1], ((0, 0), (0, 0), (0, nx - ny)))
    faces = jnp.concatenate(
        [
            fit(material[:, :, ny - 1]),
            fit(material[:, nx - 1]),
            fit(jnp.concatenate([jnp.swapaxes(mz, 1, 2).reshape(2, -1), mzx.reshape(2, -1)], 1)),
            jnp.zeros((2, width), F32),
        ],
        axis=0,
    )
    shapes, keeps = stage_shapes()
    anyspace = pl.BlockSpec(memory_space=pl.ANY)
    vmem = pl.BlockSpec(memory_space=pltpu.VMEM)
    kernel = lambda *refs: local_kernel(
        (nx, ny, nz, cols, count["gx"], count["gy"]), 0.5 / cells, *refs
    )
    return pl.pallas_call(
        kernel,
        out_shape=[jax.ShapeDtypeStruct((4, cols), F32)] * 2,
        in_specs=[anyspace] + [vmem] * 8,
        out_specs=[vmem] * 2,
        scratch_shapes=[
            pltpu.VMEM((nx, ny, nz, cols), BF16),
            pltpu.VMEM((nx // 2, cols, 2 * n), BF16),
            pltpu.VMEM((6, cols, 2 * n), F32),
            pltpu.VMEM((2, 2 * cols, 2 * n), BF16),
            pltpu.VMEM((2, cols, cols), F32),
            pltpu.VMEM((nx + 3, nz, cols), BF16),
            pltpu.VMEM((ny, nz, cols), BF16),
            pltpu.VMEM((ny + 8, nx, cols), BF16),
            pltpu.VMEM((13, 8, width), F32),
            pltpu.SemaphoreType.DMA((nx,)),
            pltpu.SemaphoreType.DMA((26,)),
            pltpu.SemaphoreType.DMA((26,)),
            pltpu.VMEM((2, 2, 4, 4, 2, 8, cols), F32),
            pltpu.SemaphoreType.DMA((10 * tiles,)),
            pltpu.SemaphoreType.DMA((10 * tiles,)),
        ]
        + [pltpu.VMEM(x, F32) for row in shapes + keeps for x in row],
        compiler_params=pltpu.CompilerParams(
            collective_id=0, has_side_effects=True, vmem_limit_bytes=63 * 1024 * 1024
        ),
        name="local_sums",
    )(eigvecs, flat, faces, zf, zx, plane, wy, wx, wz)


def per_device(eigvecs, material):
    return tuple(local_sums(eigvecs, material))


def solution(mesh):
    return jax.shard_map(
        per_device,
        mesh=mesh,
        in_specs=(P("gx", "gy", "gz", None), P(None, "gx", "gy", "gz")),
        out_specs=(P(("gx", "gy", "gz"), None), P(("gx", "gy", "gz"), None)),
        check_vma=False,
    )
```

```python
import jax
import jax.numpy as jnp
import numpy as np
from jax import lax
from jax.experimental import pallas as pl
from jax.experimental.pallas import tpu as pltpu
from jax.sharding import PartitionSpec as P

MESH = pl.DeviceIdType.MESH
F32, BF16 = jnp.float32, jnp.bfloat16
PC, PM = 1.0 / 16.0, 1.0 / 216.0


def taps(rows, cols, middle):
    gap = np.abs(rows[:, None] - cols[None, :])
    return np.where(gap == 0, middle, np.where(gap == 1, 1, 0))


def pair_weights(halo, own, middle):
    total = 1
    for h, o in zip(halo, own):
        total = total * taps(h, o, middle)
    return total


def grid(*axes):
    return [a.reshape(-1) for a in np.meshgrid(*axes, indexing="ij")]


def stacked(halo, own, pad):
    w = np.concatenate([pair_weights(halo, own, 2), pair_weights(halo, own, 4)], axis=1)
    w = np.concatenate([w, np.zeros((pad, w.shape[1]), w.dtype)], axis=0)
    return w.astype(np.float32)


WINDOWS = ((0, 256), (0, 384), (128, 384))
YWINDOWS = ((0, 256), (128, 384), (256, 512))
ZWINDOWS = ((0, 256),)


def banded(w, windows):
    m = w.shape[1] // 2
    found = []
    for t, (lo, hi) in enumerate(windows):
        own = np.r_[t * 128 : (t + 1) * 128, m + t * 128 : m + (t + 1) * 128]
        outside = np.delete(w[:, own], np.s_[lo:hi], axis=0)
        assert not outside.any()
        found.append(w[lo:hi][:, own])
    return np.concatenate(found)


def weight_arrays(nx, ny, nz):
    hx = nx // 2
    y, z = grid(np.arange(ny), np.arange(nz))
    plane = banded(stacked([y, z], [y, z], 0), WINDOWS)
    hxx, hzz = grid(np.arange(-1, hx + 1), np.arange(nz))
    oxx, ozz = grid(np.arange(hx), np.arange(nz))
    wy = stacked([hxx, hzz, 0 * hxx + 1], [oxx, ozz, 0 * oxx], 16)
    wy = banded(np.concatenate([np.zeros((16, wy.shape[1]), np.float32), wy]), YWINDOWS)
    far = 99
    slabs = []
    xs = np.arange(nx)
    for yy in range(ny):
        slabs.append((xs, 0 * xs + yy))
    ys = np.concatenate([np.arange(ny), far + 0 * np.arange(nx - ny)])
    first = np.where(xs == 0, 0, far)
    last = np.where(xs == nx - 1, 0, far)
    slabs += [(xs, 0 * xs - 1), (xs, 0 * xs + ny)]
    slabs += [(0 * xs - 1, ys), (0 * xs + nx, ys)]
    slabs += [(last - 1, 0 * xs - 1), (last - 1, 0 * xs + ny)]
    slabs += [(first + nx, 0 * xs - 1), (first + nx, 0 * xs + ny)]
    zx = np.concatenate([s[0] for s in slabs])
    zy = np.concatenate([s[1] for s in slabs])
    oyy, oxx = grid(np.arange(ny), np.arange(nx))
    wz = banded(stacked([zx, zy, 0 * zx + 1], [oxx, oyy, 0 * oxx], 0), ZWINDOWS)
    return plane, wy, wz


def nt(a, b):
    return lax.dot_general(a, b, (((1,), (1,)), ((), ())), preferred_element_type=F32)


def nn(a, b):
    return jnp.dot(a, b, preferred_element_type=F32)


def split(x):
    pad = jnp.zeros(((-x.shape[0]) % 16, x.shape[1]), F32)
    x = jnp.concatenate([x, pad], axis=0) if pad.shape[0] else x
    high = x.astype(BF16)
    rest = x - high.astype(F32)
    mid = rest.astype(BF16)
    low = (rest - mid.astype(F32)).astype(BF16)
    return jnp.concatenate([high, mid, low], axis=0)


def joined(x, rows):
    return (x[:rows] + x[16 : 16 + rows]) + x[32 : 32 + rows]


def exact(a, b):
    return joined(nn(split(a), b), a.shape[0])


def exact_nt(a, b):
    return joined(nt(split(a), b), a.shape[0])


ORDERS = ("yxz", "xzy", "zyx", "xyz")
GONE = {"x": "x", "y": "y", "z": "lh"}
SIZE = {"l": 2, "h": 2, "x": 4, "y": 4}
tiles = len(ORDERS)


def exchange_start(t, s, held, pick, place, device_of, send, stage):
    buf, dims = held
    dim = ORDERS[t][s]
    copies = []
    for j in range(3):
        at = lax.rem(place[dim] + j + 1, 4)
        copies.append(
            send(
                buf.at[pick(buf, dims, dim, at)], stage[s + 1][t].at[j],
                tiles + (s * tiles + t) * 3 + j, device_of(dim, at),
            )
        )
    return copies


def partners(gx, gy, gz):
    core, z = lax.rem(gx, 2), gz * 2 + gx // 2
    x, y = gy // 4, lax.rem(gy, 4)
    found = [(gx + 1 - 2 * core, gy, gz)]
    for j in range(1, 4):
        found.append((gx, x * 4 + lax.rem(y + j, 4), gz))
        found.append((gx, lax.rem(x + j, 4) * 4 + y, gz))
        zz = lax.rem(z + j, 4)
        found.append((lax.rem(zz, 2) * 2 + core, gy, zz // 2))
    return found


def stage_shapes():
    shapes, keeps = [[(2, 4, 4, 2, 8, 128)] * tiles], []
    for s in range(3):
        row, kept = [], []
        for t in range(tiles):
            gone = "".join(GONE[d] for d in ORDERS[t][: s + 1])
            left = tuple(SIZE[d] for d in "lxyh" if d not in gone) + (8, 128)
            row.append((3,) + left)
            kept.append(left)
        shapes.append(row)
        keeps.append(kept)
    return shapes, keeps[:2]


def local_kernel(
    dims, scale,
    v_ref, mat_ref, wp_any, wy_any, wz_any,
    out_ref,
    vbuf, vt, fbuf, ym, acc, hy, hx, hz, fh, vsem, send_sem, recv_sem,
    q, rsend, rrecv, faces_ref, zf_ref, zx_ref, wp_ref, wy_ref, wz_ref, wsem,
    ys, ht, hfar, owned, us, um, *rest,
):
    stage = [rest[s * tiles : (s + 1) * tiles] for s in range(4)]
    keep = [rest[(4 + s) * tiles : (5 + s) * tiles] for s in range(2)]
    nx, ny, nz, cols, ngx, ngy = dims
    n = ny * nz
    gx, gy, gz = lax.axis_index("gx"), lax.axis_index("gy"), lax.axis_index("gz")
    hx_n = nx // 2

    loads = [pltpu.make_async_copy(v_ref.at[x], vbuf.at[x], vsem.at[x]) for x in range(nx)]
    weights = [
        pltpu.make_async_copy(a, b, wsem.at[k])
        for k, (a, b) in enumerate(((wp_any, wp_ref), (wy_any, wy_ref), (wz_any, wz_ref)))
    ]
    weights[0].start()
    for load in loads:
        load.start()
    for load in weights[1:]:
        load.start()

    def zrow(k):
        return hz.at[k]

    links = [
        ((0, 1), False, v_ref.at[:, ny - 1], hy.at[pl.ds(1, nx)]),
        ((1, 1), False, v_ref.at[nx - 1, ny - 1], hy.at[0]),
        ((-1, 1), False, v_ref.at[0, ny - 1], hy.at[nx + 1]),
        ((1, 0), False, v_ref.at[nx - 1], hx),
        ((0, 0), True, zf_ref, hz.at[pl.ds(0, ny)]),
        ((0, 1), True, zf_ref.at[ny - 1], zrow(ny)),
        ((0, -1), True, zf_ref.at[0], zrow(ny + 1)),
        ((1, 0), True, zx_ref.at[1], zrow(ny + 2)),
        ((-1, 0), True, zx_ref.at[0], zrow(ny + 3)),
        ((1, 1), True, zf_ref.at[ny - 1], zrow(ny + 4)),
        ((1, -1), True, zf_ref.at[0], zrow(ny + 5)),
        ((-1, 1), True, zf_ref.at[ny - 1], zrow(ny + 6)),
        ((-1, -1), True, zf_ref.at[0], zrow(ny + 7)),
    ]

    def inside(dx, dy):
        ok = None
        for move, at, count in ((dx, gx, ngx), (dy, gy, ngy)):
            here = None
            if move == 1:
                here = at < count - 1
            if move == -1:
                here = at > 0
            if here is not None:
                ok = here if ok is None else jnp.logical_and(ok, here)
        return ok

    def both(a, b):
        return b if a is None else jnp.logical_and(a, b)

    def sends_if(link):
        (dx, dy), cut, _, _ = link
        ok = inside(dx, dy)
        return both(ok, gz == 0) if cut else ok

    def gets_if(link):
        (dx, dy), cut, _, _ = link
        ok = inside(-dx, -dy)
        return both(ok, gz == 1) if cut else ok

    hy[...] = jnp.zeros_like(hy)
    hx[...] = jnp.zeros_like(hx)
    hz[...] = jnp.zeros_like(hz)
    fh[...] = jnp.zeros_like(fh)

    barrier = pltpu.get_barrier_semaphore()
    targets = 0
    for link in links:
        (dx, dy), cut, _, _ = link
        source = (gx - dx, gy - dy, 0 if cut else gz)

        @pl.when(gets_if(link))
        def _(source=source):
            pl.semaphore_signal(barrier, inc=1, device_id=source, device_id_type=MESH)

        targets = targets + sends_if(link).astype(jnp.int32)
    for device in partners(gx, gy, gz):
        pl.semaphore_signal(barrier, inc=1, device_id=device, device_id_type=MESH)
    pl.semaphore_wait(barrier, targets + 10)

    copies = []
    for k, link in enumerate(links):
        (dx, dy), cut, source, target = link
        device = (gx + dx, gy + dy, 1 if cut else gz)
        pair = [
            pltpu.make_async_remote_copy(
                src_ref=s, dst_ref=t, send_sem=send_sem.at[2 * k + j],
                recv_sem=recv_sem.at[2 * k + j], device_id=device, device_id_type=MESH,
            )
            for j, (s, t) in enumerate(((faces_ref, fh.at[k]), (source, target)))
        ]
        copies.append(pair)
        if not cut:

            @pl.when(sends_if(link))
            def _(pair=pair):
                pair[1].start()

    kappa, rho = (
        jnp.concatenate([mat_ref[j, :, y, :] for y in range(ny)], axis=1) for j in range(2)
    )
    at_low = gz == 1
    cell = lax.broadcasted_iota(jnp.int32, (n, 128), 0)
    lane = lax.broadcasted_iota(jnp.int32, (n, 128), 1)
    edge_z = jnp.where(at_low, 0, nz - 1)
    hot = jnp.logical_and(cell == lane * nz + edge_z, lane < ny).astype(F32).astype(BF16)
    width = nx * nz
    for j, rows in enumerate((kappa, rho)):
        faces_ref[j : j + 1, :] = jnp.concatenate(
            [rows[x : x + 1, (ny - 1) * nz :] for x in range(nx)], axis=1
        )
        faces_ref[2 + j : 3 + j, :] = jnp.concatenate(
            [rows[nx - 1 :], jnp.zeros((1, width - n), F32)], axis=1
        )
        edge_rows = exact(rows, hot)
        turned = jnp.concatenate([edge_rows, jnp.zeros((128 - nx, 128), F32)], axis=0).T
        faces_ref[4 + j : 5 + j, :] = jnp.concatenate(
            [turned[y : y + 1, :nx] for y in range(ny)]
            + [edge_rows[:1, :nx], edge_rows[nx - 1 :, :nx]]
            + [jnp.zeros((1, width - (ny + 2) * nx), F32)],
            axis=1,
        )
    faces_ref[6:8, :] = jnp.zeros((2, width), F32)

    def z_edge(x, y, count):
        tall, low = vbuf[x, y, nz - 16 :, :], vbuf[x, y, :16, :]
        picked = jnp.where(at_low, low.astype(F32)[:, 0, :], tall.astype(F32)[:, 15, :])
        return picked.astype(BF16)

    def later_sends():
        for y in range(ny):
            zf_ref[y] = z_edge(slice(None), y, nx)
        zx_ref[...] = jnp.zeros_like(zx_ref)
        for j, x in enumerate((0, nx - 1)):
            zx_ref[j, :ny] = z_edge(x, slice(None), ny)
        for link, pair in zip(links, copies):

            @pl.when(sends_if(link))
            def _(link=link, pair=pair):
                pair[0].start()
                if link[1]:
                    pair[1].start()

    weights[0].wait()
    starts = np.cumsum([0] + [hi - lo for lo, hi in WINDOWS])
    zero = jnp.zeros((1, n), F32)
    filtered = jnp.concatenate(
        [
            exact(kappa[:, lo:hi], wp_ref[starts[t] : starts[t + 1], :128])
            for t, (lo, hi) in enumerate(WINDOWS)
        ],
        axis=1,
    )
    around = (
        jnp.concatenate([zero, filtered[:-1]], axis=0)
        + 2.0 * filtered
        + jnp.concatenate([filtered[1:], zero], axis=0)
    )
    diag = 0.5 * (3.5 * kappa + PC * around - 0.5 * kappa)
    coef_v = diag + 0.5 * kappa
    coef_s = PC * kappa
    coef_m = PM * rho

    def load_plane(x):
        if x < nx:
            vt[x // 2, :, (x % 2) * n : (x % 2 + 1) * n] = vbuf[x].reshape(n, cols).T

    def stage_a(x):
        if x < nx:
            load_plane(x)
            for t, (lo, hi) in enumerate(WINDOWS):
                base = (x % 2) * n
                fbuf[x % 6, :, t * 256 : (t + 1) * 256] = nn(
                    vt[x // 2, :, base + lo : base + hi], wp_ref[starts[t] : starts[t + 1]]
                )

    chunk = 32

    def stage_b(x, lo, hi):
        half = (x % 2) * n
        buf = (x // 2) % 2
        for r in range(lo, hi, chunk):
            rows = slice(r, r + chunk)
            for t in range(n // 128):
                cv, cs, cm = (
                    c[x : x + 1, t * 128 : (t + 1) * 128] for c in (coef_v, coef_s, coef_m)
                )
                at_s = slice(t * 256, t * 256 + 128)
                at_m = slice(t * 256 + 128, (t + 1) * 256)
                at_v = slice(half + t * 128, half + (t + 1) * 128)
                s = 2.0 * fbuf[x % 6, rows, at_s]
                m = 4.0 * fbuf[x % 6, rows, at_m]
                for near in (x - 1, x + 1):
                    if 0 <= near < nx:
                        s = s + fbuf[near % 6, rows, at_s]
                        m = m + fbuf[near % 6, rows, at_m]
                v = vt[x // 2, rows, at_v].astype(F32)
                ys[x // 2, rows, at_v] = (cv * v - cs * s).astype(BF16)
                ym[buf, rows, at_v] = (cm * m).astype(BF16)

    def stage_c(pair):
        if pair < 0:
            return
        part = nt(vt[pair], ym[pair % 2])
        if pair == 0:
            acc[1] = part
        else:
            acc[1] += part

    pairs = nx // 2
    for load in loads:
        load.wait()
    for x in range(3):
        stage_a(x)
    for i in range(pairs):
        for x in range(2):
            stage_a(2 * i + 3 + x)
            stage_b(2 * i + x, 0, cols)
        stage_c(i - 1)
        if i == 0:
            later_sends()
    stage_c(pairs - 1)
    for load in weights[1:]:
        load.wait()

    for k, link in enumerate(links):
        @pl.when(gets_if(link))
        def _(k=k):
            for copy in copies[k]:
                copy.wait_recv()

    def row(k, r, lo, hi):
        return fh[k, r : r + 1, lo:hi]

    def wide(x):
        return jnp.concatenate(x, axis=1)

    used = (hx_n + 2) * nz
    blank = jnp.zeros((1, 16), F32)
    edge = (nx - 1) * nz

    def group(k_at, m_at, halo, kh, rh, own, ko, ro, w_ref, windows):
        k, m = halo.shape[0], own.shape[1]
        ht[:, k_at : k_at + k] = halo.T
        owned[:, m_at : m_at + m] = own
        kc, rc = (jnp.broadcast_to(r, (128, k)).T for r in (kh, rh))
        far = jnp.zeros((1, k), F32)
        first = 0
        for t, (lo, hi) in enumerate(windows):
            tile = w_ref[first : first + hi - lo]
            first += hi - lo
            lanes = slice(t * 128, (t + 1) * 128)
            wc, wm = tile[:, :128].astype(F32), tile[:, 128:].astype(F32)
            ls = (wc * ((-PC) * (kc[lo:hi] + ko[:, lanes]))).astype(BF16)
            lm = (wm * (PM * (rc[lo:hi] + ro[:, lanes]))).astype(BF16)
            fbuf[t, :, :256] = nn(
                ht[:, k_at + lo : k_at + hi], jnp.concatenate([ls, lm], axis=1)
            )
            own_diag = (0.5 * PC) * jnp.sum(wc * kc[lo:hi], axis=0, keepdims=True)
            part = (0.5 * PC) * exact_nt(ko[:, lanes], tile[:, :128])
            sides = [jnp.zeros((1, lo), F32), part, jnp.zeros((1, k - hi), F32)]
            far = far + wide([x for x in sides if x.shape[1]])
            at = slice(m_at + t * 128, m_at + (t + 1) * 128)
            for r in range(0, cols, 64):
                rows = slice(r, r + 64)
                us[rows, at] = (
                    own_diag * owned[rows, at].astype(F32) + fbuf[t, rows, :128]
                ).astype(BF16)
                um[rows, at] = fbuf[t, rows, 128:256].astype(BF16)
        for r in range(0, cols, 32):
            rows = slice(r, r + 32)
            at = slice(k_at, k_at + k)
            hfar[rows, at] = (far * ht[rows, at].astype(F32)).astype(BF16)

    ky = 2 * 16 + used
    for side in range(2):
        if side == 0:
            pick = lambda r: wide(
                [blank, row(1, r, edge, edge + nz), row(0, r, 0, used - nz), blank]
            )
        else:
            pick = lambda r: wide(
                [blank, row(0, r, (hx_n - 1) * nz, nx * nz), row(2, r, 0, nz), blank]
            )
        start = side * hx_n
        none = jnp.zeros((16, cols), BF16)
        halo = jnp.concatenate(
            [none, hy[start : start + hx_n + 2].reshape(used, cols), none], axis=0
        )
        own = vbuf[start : start + hx_n, 0].reshape(hx_n * nz, cols).T
        mine = [
            wide([rows[x : x + 1, :nz] for x in range(start, start + hx_n)])
            for rows in (kappa, rho)
        ]
        group(side * ky, side * n, halo, pick(0), pick(1), own, mine[0], mine[1], wy_ref, YWINDOWS)

    group(
        2 * ky, 2 * n, hx[...].reshape(n, cols), row(3, 2, 0, n), row(3, 3, 0, n),
        vt[0, :, :n], kappa[:1], rho[:1], wp_ref, WINDOWS,
    )

    nf = nx * ny
    low, high = (nf - nx, nf), (0, nx)

    def zpick(r):
        spans = [(4, (0, nf)), (5, low), (6, high), (7, (nf + nx, nf + 2 * nx)),
                 (8, (nf, nf + nx)), (9, low), (10, high), (11, low), (12, high)]
        return wide([row(k, r, lo, hi) for k, (lo, hi) in spans])

    group(
        2 * ky + n, 3 * n, hz[...].reshape((ny + 8) * nx, cols), zpick(4), zpick(5),
        zf_ref[...].reshape(nf, cols).T, faces_ref[4:5, :nf], faces_ref[5:6, :nf],
        wz_ref, ZWINDOWS,
    )

    core, zl = lax.rem(gx, 2), gx // 2
    place = {"x": gy // 4, "y": lax.rem(gy, 4), "z": gz * 2 + zl}

    def device_of(dim, at):
        x, y, z = (at if dim == d else place[d] for d in "xyz")
        return (lax.rem(z, 2) * 2 + core, x * 4 + y, z // 2)

    pending = []

    def send(source, target, sem, device):
        copy = pltpu.make_async_remote_copy(
            src_ref=source, dst_ref=target, send_sem=rsend.at[sem], recv_sem=rrecv.at[sem],
            device_id=device, device_id_type=MESH,
        )
        copy.start()
        pending.append(copy)
        return copy

    def pick_part(buf, dims, dim, at):
        index = []
        for d in dims:
            hit = {"l": lax.rem(at, 2), "h": at // 2}.get(d) if dim == "z" else at if d == dim else None
            index.append(slice(None) if hit is None else hit)
        return tuple(index)

    half = cols // 2
    low_rows = lax.broadcasted_iota(jnp.int32, (16, 8, half), 1) < 4

    def symmetrize(h):
        for b in range(4):
            block = slice(b * 128, (b + 1) * 128)
            total = (acc[h, block] + acc[h, :, block].T) * scale
            left, right = total[:, :half].reshape(16, 8, half), total[:, half:].reshape(16, 8, half)
            first = jnp.where(low_rows, left, pltpu.roll(right, 4, 1))
            second = jnp.where(low_rows, pltpu.roll(left, 4, 1), right)
            q[h, b // 2, b % 2, :, :, 0] = first.reshape(4, 4, 8, half)
            q[h, b // 2, b % 2, :, :, 1] = second.reshape(4, 4, 8, half)

    matrix = (1, 1, 0, 0)
    held = [None] * tiles

    def swap(t):
        lanes = slice((t % 2) * 128, (t % 2 + 1) * 128)
        held[t] = send(
            q.at[matrix[t], :, 1 - core, :, :, :, :, lanes], stage[0][t], t,
            (zl * 2 + 1 - core, gy, gz),
        )

    def swapped(t):
        lanes = slice((t % 2) * 128, (t % 2 + 1) * 128)
        held[t].wait_recv()
        stage[0][t][...] += q[matrix[t], :, core, :, :, :, :, lanes]
        buf = (stage[0][t], "lxyh")
        held[t] = (buf, exchange_start(t, 0, buf, pick_part, place, device_of, send, stage))

    def advance(t, s):
        (buf, dims), copies_t = held[t]
        dim = ORDERS[t][s]
        total = buf[pick_part(buf, dims, dim, place[dim])]
        for j, copy in enumerate(copies_t):
            copy.wait_recv()
            total = total + stage[s + 1][t][j]
        if s == 2:
            rows = slice(4 * matrix[t], 4 * matrix[t] + 4)
            out_ref[rows, (t % 2) * 128 : (t % 2 + 1) * 128] = total[:4]
            out_ref[rows, half + (t % 2) * 128 : half + (t % 2 + 1) * 128] = total[4:]
            return
        kept = keep[s][t]
        kept[...] = total
        buf = (kept, "".join(d for d in dims if d not in GONE[dim]))
        held[t] = (buf, exchange_start(t, s + 1, buf, pick_part, place, device_of, send, stage))

    acc[1] += nt(owned[...], um[...])
    symmetrize(1)
    swap(0)
    swap(1)
    acc[0] = nt(owned[...], us[...])
    acc[0] += nt(ht[...], hfar[...])
    for pair in range(pairs):
        acc[0] += nt(vt[pair], ys[pair])
        if pair == 1:
            swapped(0)
            swapped(1)
    symmetrize(0)
    swap(2)
    swap(3)
    swapped(2)
    swapped(3)
    for s in range(3):
        for t in range(tiles):
            advance(t, s)
    for copy in pending:
        copy.wait_send()
    for k, link in enumerate(links):
        @pl.when(sends_if(link))
        def _(k=k):
            for copy in copies[k]:
                copy.wait_send()


def local_sums(eigvecs, material):
    nx, ny, nz, cols = eigvecs.shape
    n = ny * nz
    count = {a: lax.axis_size(a) for a in ("gx", "gy", "gz")}
    cells = nx * ny * nz * count["gx"] * count["gy"] * count["gz"]
    plane, wy, wz = (jnp.asarray(w, BF16) for w in weight_arrays(nx, ny, nz))
    width = nx * nz
    shapes, keeps = stage_shapes()
    own_cells = 3 * n + nx * ny
    halo_cells = 2 * (32 + (nx // 2 + 2) * nz) + n + (ny + 8) * nx
    anyspace = pl.BlockSpec(memory_space=pl.ANY)
    vmem = pl.BlockSpec(memory_space=pltpu.VMEM)
    kernel = lambda *refs: local_kernel(
        (nx, ny, nz, cols, count["gx"], count["gy"]), 0.5 / cells, *refs
    )
    return pl.pallas_call(
        kernel,
        out_shape=jax.ShapeDtypeStruct((8, cols), F32),
        in_specs=[anyspace, vmem] + [anyspace] * 3,
        out_specs=vmem,
        scratch_shapes=[
            pltpu.VMEM((nx, ny, nz, cols), BF16),
            pltpu.VMEM((nx // 2, cols, 2 * n), BF16),
            pltpu.VMEM((6, cols, 2 * n), F32),
            pltpu.VMEM((2, cols, 2 * n), BF16),
            pltpu.VMEM((2, cols, cols), F32),
            pltpu.VMEM((nx + 3, nz, cols), BF16),
            pltpu.VMEM((ny, nz, cols), BF16),
            pltpu.VMEM((ny + 8, nx, cols), BF16),
            pltpu.VMEM((13, 8, width), F32),
            pltpu.SemaphoreType.DMA((nx,)),
            pltpu.SemaphoreType.DMA((26,)),
            pltpu.SemaphoreType.DMA((26,)),
            pltpu.VMEM((2, 2, 2, 4, 4, 2, 8, cols // 2), F32),
            pltpu.SemaphoreType.DMA((10 * tiles,)),
            pltpu.SemaphoreType.DMA((10 * tiles,)),
            pltpu.VMEM((8, width), F32),
            pltpu.VMEM((ny, nx, cols), BF16),
            pltpu.VMEM((2, nx, cols), BF16),
            pltpu.VMEM(plane.shape, BF16),
            pltpu.VMEM(wy.shape, BF16),
            pltpu.VMEM(wz.shape, BF16),
            pltpu.SemaphoreType.DMA((3,)),
            pltpu.VMEM((nx // 2, cols, 2 * n), BF16),
            pltpu.VMEM((cols, halo_cells), BF16),
            pltpu.VMEM((cols, halo_cells), BF16),
        ]
        + [pltpu.VMEM((cols, own_cells), BF16)] * 3
        + [pltpu.VMEM(x, F32) for row in shapes + keeps for x in row],
        compiler_params=pltpu.CompilerParams(
            collective_id=0, has_side_effects=True, vmem_limit_bytes=63 * 1024 * 1024
        ),
        name="local_sums",
    )(eigvecs, material, plane, wy, wz)


def per_device(eigvecs, material):
    both = local_sums(eigvecs, material)
    return both[:4], both[4:]


def solution(mesh):
    return jax.shard_map(
        per_device,
        mesh=mesh,
        in_specs=(P("gx", "gy", "gz", None), P(None, "gx", "gy", "gz")),
        out_specs=(P(("gx", "gy", "gz"), None), P(("gx", "gy", "gz"), None)),
        check_vma=False,
    )
```

```python
import jax
import jax.numpy as jnp
import numpy as np
from jax import lax
from jax.experimental import pallas as pl
from jax.experimental.pallas import tpu as pltpu
from jax.sharding import PartitionSpec as P

MESH = pl.DeviceIdType.MESH
F32, BF16 = jnp.float32, jnp.bfloat16
PC, PM = 1.0 / 16.0, 1.0 / 216.0


def taps(rows, cols, middle):
    gap = np.abs(rows[:, None] - cols[None, :])
    return np.where(gap == 0, middle, np.where(gap == 1, 1, 0))


def pair_weights(halo, own, middle):
    total = 1
    for h, o in zip(halo, own):
        total = total * taps(h, o, middle)
    return total


def grid(*axes):
    return [a.reshape(-1) for a in np.meshgrid(*axes, indexing="ij")]


def stacked(halo, own, pad):
    w = np.concatenate([pair_weights(halo, own, 2), pair_weights(halo, own, 4)], axis=1)
    w = np.concatenate([w, np.zeros((pad, w.shape[1]), w.dtype)], axis=0)
    return w.astype(np.float32)


WINDOWS = ((0, 256), (0, 384), (128, 384))
YWINDOWS = ((0, 256), (128, 384), (256, 512))
ZWINDOWS = ((0, 256),)


RELAY = 5


def banded(w, windows):
    m = w.shape[1] // 2
    found = []
    for t, (lo, hi) in enumerate(windows):
        own = np.r_[t * 128 : (t + 1) * 128, m + t * 128 : m + (t + 1) * 128]
        outside = np.delete(w[:, own], np.s_[lo:hi], axis=0)
        assert not outside.any()
        found.append(w[lo:hi][:, own])
    return np.concatenate(found)


def weight_arrays(nx, ny, nz):
    hx = nx // 2
    y, z = grid(np.arange(ny), np.arange(nz))
    plane = banded(stacked([y, z], [y, z], 0), WINDOWS)
    hxx, hzz = grid(np.arange(-1, hx + 1), np.arange(nz))
    oxx, ozz = grid(np.arange(hx), np.arange(nz))
    wy = stacked([hxx, hzz, 0 * hxx + 1], [oxx, ozz, 0 * oxx], 16)
    wy = banded(np.concatenate([np.zeros((16, wy.shape[1]), np.float32), wy]), YWINDOWS)
    far = 99
    slabs = []
    xs = np.arange(nx)
    for yy in range(ny):
        slabs.append((xs, 0 * xs + yy))
    ys = np.concatenate([np.arange(ny), far + 0 * np.arange(nx - ny)])
    first = np.where(xs == 0, 0, far)
    last = np.where(xs == nx - 1, 0, far)
    slabs += [(xs, 0 * xs - 1), (xs, 0 * xs + ny)]
    slabs += [(0 * xs - 1, ys), (0 * xs + nx, ys)]
    slabs += [(last - 1, 0 * xs - 1), (last - 1, 0 * xs + ny)]
    slabs += [(first + nx, 0 * xs - 1), (first + nx, 0 * xs + ny)]
    zx = np.concatenate([s[0] for s in slabs])
    zy = np.concatenate([s[1] for s in slabs])
    oyy, oxx = grid(np.arange(ny), np.arange(nx))
    wz = banded(stacked([zx, zy, 0 * zx + 1], [oxx, oyy, 0 * oxx], 0), ZWINDOWS)
    return plane, wy, wz


def nt(a, b):
    return lax.dot_general(a, b, (((1,), (1,)), ((), ())), preferred_element_type=F32)


def nn(a, b):
    return jnp.dot(a, b, preferred_element_type=F32)


def split(x):
    pad = jnp.zeros(((-x.shape[0]) % 16, x.shape[1]), F32)
    x = jnp.concatenate([x, pad], axis=0) if pad.shape[0] else x
    high = x.astype(BF16)
    rest = x - high.astype(F32)
    mid = rest.astype(BF16)
    low = (rest - mid.astype(F32)).astype(BF16)
    return jnp.concatenate([high, mid, low], axis=0)


def joined(x, rows):
    return (x[:rows] + x[16 : 16 + rows]) + x[32 : 32 + rows]


def exact(a, b):
    return joined(nn(split(a), b), a.shape[0])


def exact_nt(a, b):
    return joined(nt(split(a), b), a.shape[0])


ORDERS = ("yxz", "xzy", "zyx", "xyz")
GONE = {"x": "x", "y": "y", "z": "lh"}
SIZE = {"l": 2, "h": 2, "x": 4, "y": 4}
tiles = len(ORDERS)


def exchange_start(t, s, held, pick, place, device_of, send, stage):
    buf, dims = held
    dim = ORDERS[t][s]
    copies = []
    for j in range(3):
        at = lax.rem(place[dim] + j + 1, 4)
        copies.append(
            send(
                buf.at[pick(buf, dims, dim, at)], stage[s + 1][t].at[j],
                tiles + (s * tiles + t) * 3 + j, device_of(dim, at),
            )
        )
    return copies


def partners(gx, gy, gz):
    core, z = lax.rem(gx, 2), gz * 2 + gx // 2
    x, y = gy // 4, lax.rem(gy, 4)
    found = [(gx + 1 - 2 * core, gy, gz)]
    for j in range(1, 4):
        found.append((gx, x * 4 + lax.rem(y + j, 4), gz))
        found.append((gx, lax.rem(x + j, 4) * 4 + y, gz))
        zz = lax.rem(z + j, 4)
        found.append((lax.rem(zz, 2) * 2 + core, gy, zz // 2))
    return found


def stage_shapes():
    shapes, keeps = [[(2, 4, 4, 2, 8, 128)] * tiles], []
    for s in range(3):
        row, kept = [], []
        for t in range(tiles):
            gone = "".join(GONE[d] for d in ORDERS[t][: s + 1])
            left = tuple(SIZE[d] for d in "lxyh" if d not in gone) + (8, 128)
            row.append((3,) + left)
            kept.append(left)
        shapes.append(row)
        keeps.append(kept)
    return shapes, keeps[:2]


def local_kernel(
    dims, scale,
    v_ref, mat_ref, wp_any, wy_any, wz_any,
    out_ref,
    vbuf, vt, fbuf, ym, acc, hy, hx, hz, fh, vsem, send_sem, recv_sem,
    q, rsend, rrecv, faces_ref, zf_ref, zx_ref, wp_ref, wy_ref, wz_ref, wsem,
    ys, ht, hfar, owned, us, um, hu, hc, hzx, fz_ref, fhz, *rest,
):
    stage = [rest[s * tiles : (s + 1) * tiles] for s in range(4)]
    keep = [rest[(4 + s) * tiles : (5 + s) * tiles] for s in range(2)]
    nx, ny, nz, cols, ngx, ngy = dims
    n = ny * nz
    gx, gy, gz = lax.axis_index("gx"), lax.axis_index("gy"), lax.axis_index("gz")
    hx_n = nx // 2

    loads = [pltpu.make_async_copy(v_ref.at[x], vbuf.at[x], vsem.at[x]) for x in range(nx)]
    weights = [
        pltpu.make_async_copy(a, b, wsem.at[k])
        for k, (a, b) in enumerate(((wp_any, wp_ref), (wy_any, wy_ref), (wz_any, wz_ref)))
    ]
    weights[0].start()
    for load in loads:
        load.start()
    for load in weights[1:]:
        load.start()

    links = [
        ((0, 1), 0, v_ref.at[pl.ds(0, hx_n + 1), ny - 1], hy.at[pl.ds(1, hx_n + 1)]),
        ((1, 1), 0, v_ref.at[nx - 1, ny - 1], hy.at[0]),
        ((-1, 0), 0, v_ref.at[0, ny - 1], hc),
        ((1, 0), 0, v_ref.at[nx - 1], hx),
        ((0, -1), 0, v_ref.at[pl.ds(hx_n, hx_n), 0], hu),
    ]
    links = [(o, kind, [(faces_ref, fh.at[k]), (a, b)]) for k, (o, kind, a, b) in enumerate(links)]
    cut = ((0, 0), 1, [(fz_ref, fhz.at[0]), (zf_ref, hz.at[pl.ds(0, ny)]), (zx_ref, hzx)])
    relays = [
        ((0, 1), hz.at[ny - 1]), ((0, -1), hz.at[0]), ((1, 0), hzx.at[1]), ((-1, 0), hzx.at[0]),
        ((1, 1), hz.at[ny - 1]), ((1, -1), hz.at[0]), ((-1, 1), hz.at[ny - 1]), ((-1, -1), hz.at[0]),
    ]
    links = links + [cut] + [
        (o, 2, [(fhz.at[0], fhz.at[j + 1]), (a, hz.at[ny + j])]) for j, (o, a) in enumerate(relays)
    ]

    def inside(dx, dy):
        ok = None
        for move, at, count in ((dx, gx, ngx), (dy, gy, ngy)):
            here = None
            if move == 1:
                here = at < count - 1
            if move == -1:
                here = at > 0
            if here is not None:
                ok = here if ok is None else jnp.logical_and(ok, here)
        return ok

    def both(a, b):
        return b if a is None else jnp.logical_and(a, b)

    def sends_if(link):
        (dx, dy), kind, _ = link
        ok = inside(dx, dy)
        return both(ok, gz == kind - 1) if kind else ok

    def gets_if(link):
        (dx, dy), kind, _ = link
        ok = inside(-dx, -dy)
        return both(ok, gz == 1) if kind else ok

    hy[...] = jnp.zeros_like(hy)
    hx[...] = jnp.zeros_like(hx)
    hu[...] = jnp.zeros_like(hu)
    hc[...] = jnp.zeros_like(hc)
    hz[...] = jnp.zeros_like(hz)
    hzx[...] = jnp.zeros_like(hzx)
    fh[...] = jnp.zeros_like(fh)
    fhz[...] = jnp.zeros_like(fhz)

    barrier = pltpu.get_barrier_semaphore()
    targets = 0
    for link in links:
        (dx, dy), kind, _ = link
        source = (gx - dx, gy - dy, 0 if kind == 1 else gz)

        @pl.when(gets_if(link))
        def _(source=source):
            pl.semaphore_signal(barrier, inc=1, device_id=source, device_id_type=MESH)

        targets = targets + sends_if(link).astype(jnp.int32)
    for device in partners(gx, gy, gz):
        pl.semaphore_signal(barrier, inc=1, device_id=device, device_id_type=MESH)

    copies = []
    used_sems = 0
    for (dx, dy), kind, moves in links:
        device = (gx + dx, gy + dy, 1 if kind == 1 else gz)
        group_of = []
        for a, b in moves:
            group_of.append(
                pltpu.make_async_remote_copy(
                    src_ref=a, dst_ref=b, send_sem=send_sem.at[used_sems],
                    recv_sem=recv_sem.at[used_sems], device_id=device, device_id_type=MESH,
                )
            )
            used_sems += 1
        copies.append(group_of)

    def wait_if(link, k):
        @pl.when(gets_if(link))
        def _():
            for copy in copies[k]:
                copy.wait_recv()

    def relay():
        wait_if(cut, links.index(cut))
        for link, pair in zip(links, copies):
            if link[1] == 2:

                @pl.when(sends_if(link))
                def _(pair=pair):
                    for copy in pair:
                        copy.start()

    def first_sends():
        pl.semaphore_wait(barrier, targets + 10)
        for link, pair in zip(links, copies):
            if link[1] == 0:

                @pl.when(sends_if(link))
                def _(pair=pair):
                    pair[1].start()

    kappa, rho = (
        jnp.concatenate([mat_ref[j, :, y, :] for y in range(ny)], axis=1) for j in range(2)
    )
    at_low = gz == 1
    cell = lax.broadcasted_iota(jnp.int32, (n, 128), 0)
    lane = lax.broadcasted_iota(jnp.int32, (n, 128), 1)
    edge_z = jnp.where(at_low, 0, nz - 1)
    hot = jnp.logical_and(cell == lane * nz + edge_z, lane < ny).astype(F32).astype(BF16)
    width = nx * nz
    for j, rows in enumerate((kappa, rho)):
        faces_ref[j : j + 1, :] = jnp.concatenate(
            [rows[x : x + 1, (ny - 1) * nz :] for x in range(nx)], axis=1
        )
        faces_ref[4 + j : 5 + j, :] = jnp.concatenate(
            [rows[x : x + 1, :nz] for x in range(nx)], axis=1
        )
        faces_ref[2 + j : 3 + j, :] = jnp.concatenate(
            [rows[nx - 1 :], jnp.zeros((1, width - n), F32)], axis=1
        )
        edge_rows = exact(rows, hot)
        turned = jnp.concatenate([edge_rows, jnp.zeros((128 - nx, 128), F32)], axis=0).T
        fz_ref[j : j + 1, :] = jnp.concatenate(
            [turned[y : y + 1, :nx] for y in range(ny)]
            + [edge_rows[:1, :nx], edge_rows[nx - 1 :, :nx]]
            + [jnp.zeros((1, 256 - (ny + 2) * nx), F32)],
            axis=1,
        )

    faces_ref[6:, :] = jnp.zeros((2, width), F32)
    fz_ref[2:, :] = jnp.zeros((6, 256), F32)

    def z_edge(x, y, count):
        tall, low = vbuf[x, y, nz - 16 :, :], vbuf[x, y, :16, :]
        picked = jnp.where(at_low, low.astype(F32)[:, 0, :], tall.astype(F32)[:, 15, :])
        return picked.astype(BF16)

    def later_sends():
        for load in loads[5:]:
            load.wait()
        for y in range(ny):
            zf_ref[y] = z_edge(slice(None), y, nx)
        zx_ref[...] = jnp.zeros_like(zx_ref)
        for j, x in enumerate((0, nx - 1)):
            zx_ref[j, :ny] = z_edge(x, slice(None), ny)
        for link, pair in zip(links, copies):

            if link[1] < 2:

                @pl.when(sends_if(link))
                def _(link=link, pair=pair):
                    for copy in pair if link[1] else pair[:1]:
                        copy.start()

    weights[0].wait()
    starts = np.cumsum([0] + [hi - lo for lo, hi in WINDOWS])
    zero = jnp.zeros((1, n), F32)
    filtered = jnp.concatenate(
        [
            exact(kappa[:, lo:hi], wp_ref[starts[t] : starts[t + 1], :128])
            for t, (lo, hi) in enumerate(WINDOWS)
        ],
        axis=1,
    )
    around = (
        jnp.concatenate([zero, filtered[:-1]], axis=0)
        + 2.0 * filtered
        + jnp.concatenate([filtered[1:], zero], axis=0)
    )
    diag = 0.5 * (3.5 * kappa + PC * around - 0.5 * kappa)
    coef_v = diag + 0.5 * kappa
    coef_s = PC * kappa
    coef_m = PM * rho

    def load_plane(x):
        if x < nx:
            if x < 5:
                loads[x].wait()
            vt[x // 2, :, (x % 2) * n : (x % 2 + 1) * n] = vbuf[x].reshape(n, cols).T

    def stage_a(x):
        if x < nx:
            load_plane(x)
            for t, (lo, hi) in enumerate(WINDOWS):
                base = (x % 2) * n
                fbuf[x % 6, :, t * 256 : (t + 1) * 256] = nn(
                    vt[x // 2, :, base + lo : base + hi], wp_ref[starts[t] : starts[t + 1]]
                )

    chunk = 32

    def stage_b(x, lo, hi):
        half = (x % 2) * n
        buf = (x // 2) % 2
        for r in range(lo, hi, chunk):
            rows = slice(r, r + chunk)
            for t in range(n // 128):
                cv, cs, cm = (
                    c[x : x + 1, t * 128 : (t + 1) * 128] for c in (coef_v, coef_s, coef_m)
                )
                at_s = slice(t * 256, t * 256 + 128)
                at_m = slice(t * 256 + 128, (t + 1) * 256)
                at_v = slice(half + t * 128, half + (t + 1) * 128)
                s = 2.0 * fbuf[x % 6, rows, at_s]
                m = 4.0 * fbuf[x % 6, rows, at_m]
                for near in (x - 1, x + 1):
                    if 0 <= near < nx:
                        s = s + fbuf[near % 6, rows, at_s]
                        m = m + fbuf[near % 6, rows, at_m]
                v = vt[x // 2, rows, at_v].astype(F32)
                ys[x // 2, rows, at_v] = (cv * v - cs * s).astype(BF16)
                ym[buf, rows, at_v] = (cm * m).astype(BF16)

    def stage_c(pair):
        if pair < 0:
            return
        part = nt(vt[pair], ym[pair % 2])
        if pair == 0:
            acc[1] = part
        else:
            acc[1] += part

    pairs = nx // 2
    for x in range(3):
        stage_a(x)
    first_sends()
    for i in range(pairs):
        for x in range(2):
            stage_a(2 * i + 3 + x)
            stage_b(2 * i + x, 0, cols)
        stage_c(i - 1)
        if i == 0:
            later_sends()
        if i == RELAY:
            relay()
    stage_c(pairs - 1)
    for load in weights[1:]:
        load.wait()

    for k, link in enumerate(links):
        if link[1] != 1:
            wait_if(link, k)

    def row(k, r, lo, hi):
        return fh[k, r : r + 1, lo:hi]

    def wide(x):
        return jnp.concatenate(x, axis=1)

    used = (hx_n + 2) * nz
    blank = jnp.zeros((1, 16), F32)
    edge = (nx - 1) * nz

    later = []

    def group(k_at, m_at, halo, kh, rh, own, ko, ro, w_ref, windows):
        k, m = halo.shape[0], own.shape[1]
        ht[:, k_at : k_at + k] = halo.T
        owned[:, m_at : m_at + m] = own
        rc = jnp.broadcast_to(rh, (128, k)).T
        spans = np.cumsum([0] + [hi - lo for lo, hi in windows])
        for t, (lo, hi) in enumerate(windows):
            lanes = slice(t * 128, (t + 1) * 128)
            wm = w_ref[spans[t] : spans[t + 1], 128:].astype(F32)
            lm = (wm * (PM * (rc[lo:hi] + ro[:, lanes]))).astype(BF16)
            at = slice(m_at + t * 128, m_at + (t + 1) * 128)
            um[:, at] = nn(ht[:, k_at + lo : k_at + hi], lm).astype(BF16)

        def stiff():
            kc = jnp.broadcast_to(kh, (128, k)).T
            far = jnp.zeros((1, k), F32)
            for t, (lo, hi) in enumerate(windows):
                lanes = slice(t * 128, (t + 1) * 128)
                tile = w_ref[spans[t] : spans[t + 1], :128]
                wc = tile.astype(F32)
                ls = (wc * ((-PC) * (kc[lo:hi] + ko[:, lanes]))).astype(BF16)
                fbuf[t, :, :128] = nn(ht[:, k_at + lo : k_at + hi], ls)
                own_diag = (0.5 * PC) * jnp.sum(wc * kc[lo:hi], axis=0, keepdims=True)
                part = (0.5 * PC) * exact_nt(ko[:, lanes], tile)
                sides = [jnp.zeros((1, lo), F32), part, jnp.zeros((1, k - hi), F32)]
                far = far + wide([x for x in sides if x.shape[1]])
                at = slice(m_at + t * 128, m_at + (t + 1) * 128)
                for r in range(0, cols, 64):
                    rows = slice(r, r + 64)
                    us[rows, at] = (
                        own_diag * owned[rows, at].astype(F32) + fbuf[t, rows, :128]
                    ).astype(BF16)
            for r in range(0, cols, 32):
                rows = slice(r, r + 32)
                at = slice(k_at, k_at + k)
                hfar[rows, at] = (far * ht[rows, at].astype(F32)).astype(BF16)

        later.append(stiff)

    ky = 2 * 16 + used
    none = jnp.zeros((16, cols), BF16)
    lower = lambda r: wide([blank, row(1, r, edge, edge + nz), row(0, r, 0, used - nz), blank])
    group(
        0, 0, jnp.concatenate([none, hy[...].reshape(used, cols), none], axis=0),
        lower(0), lower(1), vbuf[:hx_n, 0].reshape(hx_n * nz, cols).T,
        *(wide([rows[x : x + 1, :nz] for x in range(hx_n)]) for rows in (kappa, rho)),
        wy_ref, YWINDOWS,
    )
    upper = lambda r: wide(
        [blank, faces_ref[r : r + 1, (hx_n - 1) * nz :], row(2, r, 0, nz), blank]
    )
    mine = vbuf[hx_n - 1 :, ny - 1].reshape(used - nz, cols)
    group(
        ky, n, jnp.concatenate([none, mine, hc[...], none], axis=0),
        upper(0), upper(1), hu[...].reshape(hx_n * nz, cols).T,
        row(4, 4, hx_n * nz, nx * nz), row(4, 5, hx_n * nz, nx * nz), wy_ref, YWINDOWS,
    )

    group(
        2 * ky, 2 * n, hx[...].reshape(n, cols), row(3, 2, 0, n), row(3, 3, 0, n),
        vt[0, :, :n], kappa[:1], rho[:1], wp_ref, WINDOWS,
    )

    nf = nx * ny
    low, high = (nf - nx, nf), (0, nx)

    def zpick(r):
        spans = [(0, nf), low, high, (nf + nx, nf + 2 * nx), (nf, nf + nx), low, high, low, high]
        return wide([fhz[k, r : r + 1, lo:hi] for k, (lo, hi) in enumerate(spans)])

    group(
        2 * ky + n, 3 * n, hz[...].reshape((ny + 8) * nx, cols), zpick(0), zpick(1),
        zf_ref[...].reshape(nf, cols).T, fz_ref[:1, :nf], fz_ref[1:2, :nf],
        wz_ref, ZWINDOWS,
    )

    core, zl = lax.rem(gx, 2), gx // 2
    place = {"x": gy // 4, "y": lax.rem(gy, 4), "z": gz * 2 + zl}

    def device_of(dim, at):
        x, y, z = (at if dim == d else place[d] for d in "xyz")
        return (lax.rem(z, 2) * 2 + core, x * 4 + y, z // 2)

    pending = []

    def send(source, target, sem, device):
        copy = pltpu.make_async_remote_copy(
            src_ref=source, dst_ref=target, send_sem=rsend.at[sem], recv_sem=rrecv.at[sem],
            device_id=device, device_id_type=MESH,
        )
        copy.start()
        pending.append(copy)
        return copy

    def pick_part(buf, dims, dim, at):
        index = []
        for d in dims:
            hit = {"l": lax.rem(at, 2), "h": at // 2}.get(d) if dim == "z" else at if d == dim else None
            index.append(slice(None) if hit is None else hit)
        return tuple(index)

    half = cols // 2
    low_rows = lax.broadcasted_iota(jnp.int32, (16, 8, half), 1) < 4

    def symmetrize(h):
        for b in range(4):
            block = slice(b * 128, (b + 1) * 128)
            total = (acc[h, block] + acc[h, :, block].T) * scale
            left, right = total[:, :half].reshape(16, 8, half), total[:, half:].reshape(16, 8, half)
            first = jnp.where(low_rows, left, pltpu.roll(right, 4, 1))
            second = jnp.where(low_rows, pltpu.roll(left, 4, 1), right)
            q[h, b // 2, b % 2, :, :, 0] = first.reshape(4, 4, 8, half)
            q[h, b // 2, b % 2, :, :, 1] = second.reshape(4, 4, 8, half)

    matrix = (1, 1, 0, 0)
    held = [None] * tiles

    def swap(t):
        lanes = slice((t % 2) * 128, (t % 2 + 1) * 128)
        held[t] = send(
            q.at[matrix[t], :, 1 - core, :, :, :, :, lanes], stage[0][t], t,
            (zl * 2 + 1 - core, gy, gz),
        )

    def swapped(t):
        lanes = slice((t % 2) * 128, (t % 2 + 1) * 128)
        held[t].wait_recv()
        stage[0][t][...] += q[matrix[t], :, core, :, :, :, :, lanes]
        buf = (stage[0][t], "lxyh")
        held[t] = (buf, exchange_start(t, 0, buf, pick_part, place, device_of, send, stage))

    def advance(t, s):
        (buf, dims), copies_t = held[t]
        dim = ORDERS[t][s]
        total = buf[pick_part(buf, dims, dim, place[dim])]
        for j, copy in enumerate(copies_t):
            copy.wait_recv()
            total = total + stage[s + 1][t][j]
        if s == 2:
            rows = slice(4 * matrix[t], 4 * matrix[t] + 4)
            out_ref[rows, (t % 2) * 128 : (t % 2 + 1) * 128] = total[:4]
            out_ref[rows, half + (t % 2) * 128 : half + (t % 2 + 1) * 128] = total[4:]
            return
        kept = keep[s][t]
        kept[...] = total
        buf = (kept, "".join(d for d in dims if d not in GONE[dim]))
        held[t] = (buf, exchange_start(t, s + 1, buf, pick_part, place, device_of, send, stage))

    acc[1] += nt(owned[...], um[...])
    symmetrize(1)
    swap(0)
    swap(1)
    for stiff in later:
        stiff()
    acc[0] = nt(owned[...], us[...])
    acc[0] += nt(ht[...], hfar[...])
    for pair in range(pairs):
        acc[0] += nt(vt[pair], ys[pair])
        if pair == 1:
            swapped(0)
            swapped(1)
    symmetrize(0)
    swap(2)
    swap(3)
    swapped(2)
    swapped(3)
    for s in range(3):
        for t in range(tiles):
            advance(t, s)
    for copy in pending:
        copy.wait_send()
    for k, link in enumerate(links):
        @pl.when(sends_if(link))
        def _(k=k):
            for copy in copies[k]:
                copy.wait_send()


def local_sums(eigvecs, material):
    nx, ny, nz, cols = eigvecs.shape
    n = ny * nz
    count = {a: lax.axis_size(a) for a in ("gx", "gy", "gz")}
    cells = nx * ny * nz * count["gx"] * count["gy"] * count["gz"]
    plane, wy, wz = (jnp.asarray(w, BF16) for w in weight_arrays(nx, ny, nz))
    width = nx * nz
    shapes, keeps = stage_shapes()
    own_cells = 3 * n + nx * ny
    halo_cells = 2 * (32 + (nx // 2 + 2) * nz) + n + (ny + 8) * nx
    anyspace = pl.BlockSpec(memory_space=pl.ANY)
    vmem = pl.BlockSpec(memory_space=pltpu.VMEM)
    kernel = lambda *refs: local_kernel(
        (nx, ny, nz, cols, count["gx"], count["gy"]), 0.5 / cells, *refs
    )
    return pl.pallas_call(
        kernel,
        out_shape=jax.ShapeDtypeStruct((8, cols), F32),
        in_specs=[anyspace, vmem] + [anyspace] * 3,
        out_specs=vmem,
        scratch_shapes=[
            pltpu.VMEM((nx, ny, nz, cols), BF16),
            pltpu.VMEM((nx // 2, cols, 2 * n), BF16),
            pltpu.VMEM((6, cols, 2 * n), F32),
            pltpu.VMEM((2, cols, 2 * n), BF16),
            pltpu.VMEM((2, cols, cols), F32),
            pltpu.VMEM((nx // 2 + 2, nz, cols), BF16),
            pltpu.VMEM((ny, nz, cols), BF16),
            pltpu.VMEM((ny + 8, nx, cols), BF16),
            pltpu.VMEM((5, 8, width), F32),
            pltpu.SemaphoreType.DMA((nx,)),
            pltpu.SemaphoreType.DMA((29,)),
            pltpu.SemaphoreType.DMA((29,)),
            pltpu.VMEM((2, 2, 2, 4, 4, 2, 8, cols // 2), F32),
            pltpu.SemaphoreType.DMA((10 * tiles,)),
            pltpu.SemaphoreType.DMA((10 * tiles,)),
            pltpu.VMEM((8, width), F32),
            pltpu.VMEM((ny, nx, cols), BF16),
            pltpu.VMEM((2, nx, cols), BF16),
            pltpu.VMEM(plane.shape, BF16),
            pltpu.VMEM(wy.shape, BF16),
            pltpu.VMEM(wz.shape, BF16),
            pltpu.SemaphoreType.DMA((3,)),
            pltpu.VMEM((nx // 2, cols, 2 * n), BF16),
            pltpu.VMEM((cols, halo_cells), BF16),
            pltpu.VMEM((cols, halo_cells), BF16),
        ]
        + [pltpu.VMEM((cols, own_cells), BF16)] * 3
        + [pltpu.VMEM((nx // 2, nz, cols), BF16), pltpu.VMEM((nz, cols), BF16)]
        + [pltpu.VMEM((2, nx, cols), BF16), pltpu.VMEM((8, 256), F32), pltpu.VMEM((9, 8, 256), F32)]
        + [pltpu.VMEM(x, F32) for row in shapes + keeps for x in row],
        compiler_params=pltpu.CompilerParams(
            collective_id=0, has_side_effects=True, vmem_limit_bytes=63 * 1024 * 1024
        ),
        name="local_sums",
    )(eigvecs, material, plane, wy, wz)


def per_device(eigvecs, material):
    both = local_sums(eigvecs, material)
    return both[:4], both[4:]


def solution(mesh):
    return jax.shard_map(
        per_device,
        mesh=mesh,
        in_specs=(P("gx", "gy", "gz", None), P(None, "gx", "gy", "gz")),
        out_specs=(P(("gx", "gy", "gz"), None), P(("gx", "gy", "gz"), None)),
        check_vma=False,
    )
```

```python
import jax
import jax.numpy as jnp
import numpy as np
from jax import lax
from jax.experimental import pallas as pl
from jax.experimental.pallas import tpu as pltpu
from jax.sharding import PartitionSpec as P

MESH = pl.DeviceIdType.MESH
F32, BF16 = jnp.float32, jnp.bfloat16
PC, PM = 1.0 / 16.0, 1.0 / 216.0


def taps(rows, cols, middle):
    gap = np.abs(rows[:, None] - cols[None, :])
    return np.where(gap == 0, middle, np.where(gap == 1, 1, 0))


def pair_weights(halo, own, middle):
    total = 1
    for h, o in zip(halo, own):
        total = total * taps(h, o, middle)
    return total


def grid(*axes):
    return [a.reshape(-1) for a in np.meshgrid(*axes, indexing="ij")]


def stacked(halo, own, pad):
    w = np.concatenate([pair_weights(halo, own, 2), pair_weights(halo, own, 4)], axis=1)
    w = np.concatenate([w, np.zeros((pad, w.shape[1]), w.dtype)], axis=0)
    return w.astype(np.float32)


WINDOWS = ((0, 256), (0, 384), (128, 384))
YWINDOWS = ((0, 256), (128, 384), (256, 512))
ZWINDOWS = ((0, 256),)


RELAY = 5


def banded(w, windows):
    m = w.shape[1] // 2
    found = []
    for t, (lo, hi) in enumerate(windows):
        own = np.r_[t * 128 : (t + 1) * 128, m + t * 128 : m + (t + 1) * 128]
        outside = np.delete(w[:, own], np.s_[lo:hi], axis=0)
        assert not outside.any()
        found.append(w[lo:hi][:, own])
    return np.concatenate(found)


def weight_arrays(nx, ny, nz):
    hx = nx // 2
    y, z = grid(np.arange(ny), np.arange(nz))
    plane = banded(stacked([y, z], [y, z], 0), WINDOWS)
    hxx, hzz = grid(np.arange(-1, hx + 1), np.arange(nz))
    oxx, ozz = grid(np.arange(hx), np.arange(nz))
    wy = stacked([hxx, hzz, 0 * hxx + 1], [oxx, ozz, 0 * oxx], 16)
    wy = banded(np.concatenate([np.zeros((16, wy.shape[1]), np.float32), wy]), YWINDOWS)
    far = 99
    slabs = []
    xs = np.arange(nx)
    for yy in range(ny):
        slabs.append((xs, 0 * xs + yy))
    ys = np.concatenate([np.arange(ny), far + 0 * np.arange(nx - ny)])
    first = np.where(xs == 0, 0, far)
    last = np.where(xs == nx - 1, 0, far)
    slabs += [(xs, 0 * xs - 1), (xs, 0 * xs + ny)]
    slabs += [(0 * xs - 1, ys), (0 * xs + nx, ys)]
    slabs += [(last - 1, 0 * xs - 1), (last - 1, 0 * xs + ny)]
    slabs += [(first + nx, 0 * xs - 1), (first + nx, 0 * xs + ny)]
    zx = np.concatenate([s[0] for s in slabs])
    zy = np.concatenate([s[1] for s in slabs])
    oyy, oxx = grid(np.arange(ny), np.arange(nx))
    wz = banded(stacked([zx, zy, 0 * zx + 1], [oxx, oyy, 0 * oxx], 0), ZWINDOWS)
    return plane, wy, wz


def nt(a, b):
    return lax.dot_general(a, b, (((1,), (1,)), ((), ())), preferred_element_type=F32)


def nn(a, b):
    return jnp.dot(a, b, preferred_element_type=F32)


def split(x):
    pad = jnp.zeros(((-x.shape[0]) % 16, x.shape[1]), F32)
    x = jnp.concatenate([x, pad], axis=0) if pad.shape[0] else x
    high = x.astype(BF16)
    rest = x - high.astype(F32)
    mid = rest.astype(BF16)
    low = (rest - mid.astype(F32)).astype(BF16)
    return jnp.concatenate([high, mid, low], axis=0)


def joined(x, rows):
    return (x[:rows] + x[16 : 16 + rows]) + x[32 : 32 + rows]


def exact(a, b):
    return joined(nn(split(a), b), a.shape[0])


def exact_nt(a, b):
    return joined(nt(split(a), b), a.shape[0])


ORDERS = ("yxz", "xzy", "zyx", "xyz")
GONE = {"x": "x", "y": "y", "z": "lh"}
SIZE = {"l": 2, "h": 2, "x": 4, "y": 4}
tiles = len(ORDERS)


def exchange_start(t, s, held, pick, place, device_of, send, stage):
    buf, dims = held
    dim = ORDERS[t][s]
    copies = []
    for j in range(3):
        at = lax.rem(place[dim] + j + 1, 4)
        copies.append(
            send(
                buf.at[pick(buf, dims, dim, at)], stage[s + 1][t].at[j],
                tiles + (s * tiles + t) * 3 + j, device_of(dim, at),
            )
        )
    return copies


def partners(gx, gy, gz):
    core, z = lax.rem(gx, 2), gz * 2 + gx // 2
    x, y = gy // 4, lax.rem(gy, 4)
    found = [(gx + 1 - 2 * core, gy, gz)]
    for j in range(1, 4):
        found.append((gx, x * 4 + lax.rem(y + j, 4), gz))
        found.append((gx, lax.rem(x + j, 4) * 4 + y, gz))
        zz = lax.rem(z + j, 4)
        found.append((lax.rem(zz, 2) * 2 + core, gy, zz // 2))
    return found


def stage_shapes():
    shapes, keeps = [[(2, 4, 4, 2, 8, 128)] * tiles], []
    for s in range(3):
        row, kept = [], []
        for t in range(tiles):
            gone = "".join(GONE[d] for d in ORDERS[t][: s + 1])
            left = tuple(SIZE[d] for d in "lxyh" if d not in gone) + (8, 128)
            row.append((3,) + left)
            kept.append(left)
        shapes.append(row)
        keeps.append(kept)
    return shapes, keeps[:2]


def local_kernel(
    dims, scale,
    v_ref, mat_ref, wp_any, wy_any, wz_any,
    out_ref,
    vbuf, vt, fbuf, ym, acc, hy, hx, hz, fh, vsem, send_sem, recv_sem,
    q, rsend, rrecv, faces_ref, zf_ref, zx_ref, wp_ref, wy_ref, wz_ref, wsem,
    ys, ht, hfar, owned, us, um, hu, hc, hzx, fz_ref, fhz, *rest,
):
    stage = [rest[s * tiles : (s + 1) * tiles] for s in range(4)]
    keep = [rest[(4 + s) * tiles : (5 + s) * tiles] for s in range(2)]
    nx, ny, nz, cols, ngx, ngy = dims
    n = ny * nz
    gx, gy, gz = lax.axis_index("gx"), lax.axis_index("gy"), lax.axis_index("gz")
    hx_n = nx // 2

    loads = [pltpu.make_async_copy(v_ref.at[x], vbuf.at[x], vsem.at[x]) for x in range(nx)]
    weights = [
        pltpu.make_async_copy(a, b, wsem.at[k])
        for k, (a, b) in enumerate(((wp_any, wp_ref), (wy_any, wy_ref), (wz_any, wz_ref)))
    ]
    weights[0].start()
    for load in loads:
        load.start()
    for load in weights[1:]:
        load.start()

    links = [
        ((0, 1), 0, v_ref.at[pl.ds(0, hx_n + 1), ny - 1], hy.at[pl.ds(1, hx_n + 1)]),
        ((1, 1), 0, v_ref.at[nx - 1, ny - 1], hy.at[0]),
        ((-1, 0), 0, v_ref.at[0, ny - 1], hc),
        ((1, 0), 0, v_ref.at[nx - 1], hx),
        ((0, -1), 0, v_ref.at[pl.ds(hx_n, hx_n), 0], hu),
    ]
    links = [(o, kind, [(faces_ref, fh.at[k]), (a, b)]) for k, (o, kind, a, b) in enumerate(links)]
    cut = ((0, 0), 1, [(fz_ref, fhz.at[0]), (zf_ref, hz.at[pl.ds(0, ny)]), (zx_ref, hzx)])
    relays = [
        ((0, 1), hz.at[ny - 1]), ((0, -1), hz.at[0]), ((1, 0), hzx.at[1]), ((-1, 0), hzx.at[0]),
        ((1, 1), hz.at[ny - 1]), ((1, -1), hz.at[0]), ((-1, 1), hz.at[ny - 1]), ((-1, -1), hz.at[0]),
    ]
    links = links + [cut] + [
        (o, 2, [(fhz.at[0], fhz.at[j + 1]), (a, hz.at[ny + j])]) for j, (o, a) in enumerate(relays)
    ]

    def inside(dx, dy):
        ok = None
        for move, at, count in ((dx, gx, ngx), (dy, gy, ngy)):
            here = None
            if move == 1:
                here = at < count - 1
            if move == -1:
                here = at > 0
            if here is not None:
                ok = here if ok is None else jnp.logical_and(ok, here)
        return ok

    def both(a, b):
        return b if a is None else jnp.logical_and(a, b)

    def sends_if(link):
        (dx, dy), kind, _ = link
        ok = inside(dx, dy)
        return both(ok, gz == kind - 1) if kind else ok

    def gets_if(link):
        (dx, dy), kind, _ = link
        ok = inside(-dx, -dy)
        return both(ok, gz == 1) if kind else ok

    hy[...] = jnp.zeros_like(hy)
    hx[...] = jnp.zeros_like(hx)
    hu[...] = jnp.zeros_like(hu)
    hc[...] = jnp.zeros_like(hc)
    hz[...] = jnp.zeros_like(hz)
    hzx[...] = jnp.zeros_like(hzx)
    fh[...] = jnp.zeros_like(fh)
    fhz[...] = jnp.zeros_like(fhz)

    barrier = pltpu.get_barrier_semaphore()
    targets = 0
    for link in links:
        (dx, dy), kind, _ = link
        source = (gx - dx, gy - dy, 0 if kind == 1 else gz)

        @pl.when(gets_if(link))
        def _(source=source):
            pl.semaphore_signal(barrier, inc=1, device_id=source, device_id_type=MESH)

        targets = targets + sends_if(link).astype(jnp.int32)
    for device in partners(gx, gy, gz):
        pl.semaphore_signal(barrier, inc=1, device_id=device, device_id_type=MESH)

    copies = []
    used_sems = 0
    for (dx, dy), kind, moves in links:
        device = (gx + dx, gy + dy, 1 if kind == 1 else gz)
        group_of = []
        for a, b in moves:
            group_of.append(
                pltpu.make_async_remote_copy(
                    src_ref=a, dst_ref=b, send_sem=send_sem.at[used_sems],
                    recv_sem=recv_sem.at[used_sems], device_id=device, device_id_type=MESH,
                )
            )
            used_sems += 1
        copies.append(group_of)

    def wait_if(link, k):
        @pl.when(gets_if(link))
        def _():
            for copy in copies[k]:
                copy.wait_recv()

    def relay():
        wait_if(cut, links.index(cut))
        for link, pair in zip(links, copies):
            if link[1] == 2:

                @pl.when(sends_if(link))
                def _(pair=pair):
                    for copy in pair:
                        copy.start()

    def first_sends():
        pl.semaphore_wait(barrier, targets + 10)
        for link, pair in zip(links, copies):
            if link[1] == 0:

                @pl.when(sends_if(link))
                def _(pair=pair):
                    pair[1].start()

    first_sends()
    kappa, rho = (
        jnp.concatenate([mat_ref[j, :, y, :] for y in range(ny)], axis=1) for j in range(2)
    )
    at_low = gz == 1
    cell = lax.broadcasted_iota(jnp.int32, (n, 128), 0)
    lane = lax.broadcasted_iota(jnp.int32, (n, 128), 1)
    edge_z = jnp.where(at_low, 0, nz - 1)
    hot = jnp.logical_and(cell == lane * nz + edge_z, lane < ny).astype(F32).astype(BF16)
    width = nx * nz
    for j, rows in enumerate((kappa, rho)):
        faces_ref[j : j + 1, :] = jnp.concatenate(
            [rows[x : x + 1, (ny - 1) * nz :] for x in range(nx)], axis=1
        )
        faces_ref[4 + j : 5 + j, :] = jnp.concatenate(
            [rows[x : x + 1, :nz] for x in range(nx)], axis=1
        )
        faces_ref[2 + j : 3 + j, :] = jnp.concatenate(
            [rows[nx - 1 :], jnp.zeros((1, width - n), F32)], axis=1
        )
        edge_rows = exact(rows, hot)
        turned = jnp.concatenate([edge_rows, jnp.zeros((128 - nx, 128), F32)], axis=0).T
        fz_ref[j : j + 1, :] = jnp.concatenate(
            [turned[y : y + 1, :nx] for y in range(ny)]
            + [edge_rows[:1, :nx], edge_rows[nx - 1 :, :nx]]
            + [jnp.zeros((1, 256 - (ny + 2) * nx), F32)],
            axis=1,
        )

    faces_ref[6:, :] = jnp.zeros((2, width), F32)
    fz_ref[2:, :] = jnp.zeros((6, 256), F32)

    def z_edge(x, y, count):
        tall, low = vbuf[x, y, nz - 16 :, :], vbuf[x, y, :16, :]
        picked = jnp.where(at_low, low.astype(F32)[:, 0, :], tall.astype(F32)[:, 15, :])
        return picked.astype(BF16)

    def later_sends():
        for load in loads[5:]:
            load.wait()
        for y in range(ny):
            zf_ref[y] = z_edge(slice(None), y, nx)
        zx_ref[...] = jnp.zeros_like(zx_ref)
        for j, x in enumerate((0, nx - 1)):
            zx_ref[j, :ny] = z_edge(x, slice(None), ny)
        for link, pair in zip(links, copies):

            if link[1] < 2:

                @pl.when(sends_if(link))
                def _(link=link, pair=pair):
                    for copy in pair if link[1] else pair[:1]:
                        copy.start()

    weights[0].wait()
    starts = np.cumsum([0] + [hi - lo for lo, hi in WINDOWS])
    zero = jnp.zeros((1, n), F32)
    filtered = jnp.concatenate(
        [
            exact(kappa[:, lo:hi], wp_ref[starts[t] : starts[t + 1], :128])
            for t, (lo, hi) in enumerate(WINDOWS)
        ],
        axis=1,
    )
    around = (
        jnp.concatenate([zero, filtered[:-1]], axis=0)
        + 2.0 * filtered
        + jnp.concatenate([filtered[1:], zero], axis=0)
    )
    diag = 0.5 * (3.5 * kappa + PC * around - 0.5 * kappa)
    coef_v = diag + 0.5 * kappa
    coef_s = PC * kappa
    coef_m = PM * rho

    def load_plane(x):
        if x < nx:
            if x < 5:
                loads[x].wait()
            vt[x // 2, :, (x % 2) * n : (x % 2 + 1) * n] = vbuf[x].reshape(n, cols).T

    def stage_a(x):
        if x < nx:
            load_plane(x)
            for t, (lo, hi) in enumerate(WINDOWS):
                base = (x % 2) * n
                fbuf[x % 6, :, t * 256 : (t + 1) * 256] = nn(
                    vt[x // 2, :, base + lo : base + hi], wp_ref[starts[t] : starts[t + 1]]
                )

    chunk = 32

    def stage_b(x, lo, hi):
        half = (x % 2) * n
        buf = (x // 2) % 2
        for r in range(lo, hi, chunk):
            rows = slice(r, r + chunk)
            for t in range(n // 128):
                cv, cs, cm = (
                    c[x : x + 1, t * 128 : (t + 1) * 128] for c in (coef_v, coef_s, coef_m)
                )
                at_s = slice(t * 256, t * 256 + 128)
                at_m = slice(t * 256 + 128, (t + 1) * 256)
                at_v = slice(half + t * 128, half + (t + 1) * 128)
                s = 2.0 * fbuf[x % 6, rows, at_s]
                m = 4.0 * fbuf[x % 6, rows, at_m]
                for near in (x - 1, x + 1):
                    if 0 <= near < nx:
                        s = s + fbuf[near % 6, rows, at_s]
                        m = m + fbuf[near % 6, rows, at_m]
                v = vt[x // 2, rows, at_v].astype(F32)
                ys[x // 2, rows, at_v] = (cv * v - cs * s).astype(BF16)
                ym[buf, rows, at_v] = (cm * m).astype(BF16)

    def stage_c(pair):
        if pair < 0:
            return
        part = nt(vt[pair], ym[pair % 2])
        if pair == 0:
            acc[1] = part
        else:
            acc[1] += part

    pairs = nx // 2
    for x in range(3):
        stage_a(x)
    for i in range(pairs):
        for x in range(2):
            stage_a(2 * i + 3 + x)
            stage_b(2 * i + x, 0, cols)
        stage_c(i - 1)
        if i == 0:
            later_sends()
        if i == RELAY:
            relay()
    stage_c(pairs - 1)
    for load in weights[1:]:
        load.wait()

    for k, link in enumerate(links):
        if link[1] != 1:
            wait_if(link, k)

    def row(k, r, lo, hi):
        return fh[k, r : r + 1, lo:hi]

    def wide(x):
        return jnp.concatenate(x, axis=1)

    used = (hx_n + 2) * nz
    blank = jnp.zeros((1, 16), F32)
    edge = (nx - 1) * nz

    later = []

    def group(k_at, m_at, halo, kh, rh, own, ko, ro, w_ref, windows):
        k, m = halo.shape[0], own.shape[1]
        ht[:, k_at : k_at + k] = halo.T
        owned[:, m_at : m_at + m] = own
        rc = jnp.broadcast_to(rh, (128, k)).T
        spans = np.cumsum([0] + [hi - lo for lo, hi in windows])
        for t, (lo, hi) in enumerate(windows):
            lanes = slice(t * 128, (t + 1) * 128)
            wm = w_ref[spans[t] : spans[t + 1], 128:].astype(F32)
            lm = (wm * (PM * (rc[lo:hi] + ro[:, lanes]))).astype(BF16)
            at = slice(m_at + t * 128, m_at + (t + 1) * 128)
            um[:, at] = nn(ht[:, k_at + lo : k_at + hi], lm).astype(BF16)

        def stiff():
            kc = jnp.broadcast_to(kh, (128, k)).T
            far = jnp.zeros((1, k), F32)
            for t, (lo, hi) in enumerate(windows):
                lanes = slice(t * 128, (t + 1) * 128)
                tile = w_ref[spans[t] : spans[t + 1], :128]
                wc = tile.astype(F32)
                ls = (wc * ((-PC) * (kc[lo:hi] + ko[:, lanes]))).astype(BF16)
                fbuf[t, :, :128] = nn(ht[:, k_at + lo : k_at + hi], ls)
                own_diag = (0.5 * PC) * jnp.sum(wc * kc[lo:hi], axis=0, keepdims=True)
                part = (0.5 * PC) * exact_nt(ko[:, lanes], tile)
                sides = [jnp.zeros((1, lo), F32), part, jnp.zeros((1, k - hi), F32)]
                far = far + wide([x for x in sides if x.shape[1]])
                at = slice(m_at + t * 128, m_at + (t + 1) * 128)
                for r in range(0, cols, 64):
                    rows = slice(r, r + 64)
                    us[rows, at] = (
                        own_diag * owned[rows, at].astype(F32) + fbuf[t, rows, :128]
                    ).astype(BF16)
            for r in range(0, cols, 32):
                rows = slice(r, r + 32)
                at = slice(k_at, k_at + k)
                hfar[rows, at] = (far * ht[rows, at].astype(F32)).astype(BF16)

        later.append(stiff)

    ky = 2 * 16 + used
    none = jnp.zeros((16, cols), BF16)
    lower = lambda r: wide([blank, row(1, r, edge, edge + nz), row(0, r, 0, used - nz), blank])
    group(
        0, 0, jnp.concatenate([none, hy[...].reshape(used, cols), none], axis=0),
        lower(0), lower(1), vbuf[:hx_n, 0].reshape(hx_n * nz, cols).T,
        *(wide([rows[x : x + 1, :nz] for x in range(hx_n)]) for rows in (kappa, rho)),
        wy_ref, YWINDOWS,
    )
    upper = lambda r: wide(
        [blank, faces_ref[r : r + 1, (hx_n - 1) * nz :], row(2, r, 0, nz), blank]
    )
    mine = vbuf[hx_n - 1 :, ny - 1].reshape(used - nz, cols)
    group(
        ky, n, jnp.concatenate([none, mine, hc[...], none], axis=0),
        upper(0), upper(1), hu[...].reshape(hx_n * nz, cols).T,
        row(4, 4, hx_n * nz, nx * nz), row(4, 5, hx_n * nz, nx * nz), wy_ref, YWINDOWS,
    )

    group(
        2 * ky, 2 * n, hx[...].reshape(n, cols), row(3, 2, 0, n), row(3, 3, 0, n),
        vt[0, :, :n], kappa[:1], rho[:1], wp_ref, WINDOWS,
    )

    nf = nx * ny
    low, high = (nf - nx, nf), (0, nx)

    def zpick(r):
        spans = [(0, nf), low, high, (nf + nx, nf + 2 * nx), (nf, nf + nx), low, high, low, high]
        return wide([fhz[k, r : r + 1, lo:hi] for k, (lo, hi) in enumerate(spans)])

    group(
        2 * ky + n, 3 * n, hz[...].reshape((ny + 8) * nx, cols), zpick(0), zpick(1),
        zf_ref[...].reshape(nf, cols).T, fz_ref[:1, :nf], fz_ref[1:2, :nf],
        wz_ref, ZWINDOWS,
    )

    core, zl = lax.rem(gx, 2), gx // 2
    place = {"x": gy // 4, "y": lax.rem(gy, 4), "z": gz * 2 + zl}

    def device_of(dim, at):
        x, y, z = (at if dim == d else place[d] for d in "xyz")
        return (lax.rem(z, 2) * 2 + core, x * 4 + y, z // 2)

    pending = []

    def send(source, target, sem, device):
        copy = pltpu.make_async_remote_copy(
            src_ref=source, dst_ref=target, send_sem=rsend.at[sem], recv_sem=rrecv.at[sem],
            device_id=device, device_id_type=MESH,
        )
        copy.start()
        pending.append(copy)
        return copy

    def pick_part(buf, dims, dim, at):
        index = []
        for d in dims:
            hit = {"l": lax.rem(at, 2), "h": at // 2}.get(d) if dim == "z" else at if d == dim else None
            index.append(slice(None) if hit is None else hit)
        return tuple(index)

    half = cols // 2
    low_rows = lax.broadcasted_iota(jnp.int32, (16, 8, half), 1) < 4

    def symmetrize(h):
        for b in range(4):
            block = slice(b * 128, (b + 1) * 128)
            total = (acc[h, block] + acc[h, :, block].T) * scale
            left, right = total[:, :half].reshape(16, 8, half), total[:, half:].reshape(16, 8, half)
            first = jnp.where(low_rows, left, pltpu.roll(right, 4, 1))
            second = jnp.where(low_rows, pltpu.roll(left, 4, 1), right)
            q[h, b // 2, b % 2, :, :, 0] = first.reshape(4, 4, 8, half)
            q[h, b // 2, b % 2, :, :, 1] = second.reshape(4, 4, 8, half)

    matrix = (1, 1, 0, 0)
    held = [None] * tiles

    def swap(t):
        lanes = slice((t % 2) * 128, (t % 2 + 1) * 128)
        held[t] = send(
            q.at[matrix[t], :, 1 - core, :, :, :, :, lanes], stage[0][t], t,
            (zl * 2 + 1 - core, gy, gz),
        )

    def swapped(t):
        lanes = slice((t % 2) * 128, (t % 2 + 1) * 128)
        held[t].wait_recv()
        stage[0][t][...] += q[matrix[t], :, core, :, :, :, :, lanes]
        buf = (stage[0][t], "lxyh")
        held[t] = (buf, exchange_start(t, 0, buf, pick_part, place, device_of, send, stage))

    def advance(t, s):
        (buf, dims), copies_t = held[t]
        dim = ORDERS[t][s]
        total = buf[pick_part(buf, dims, dim, place[dim])]
        for j, copy in enumerate(copies_t):
            copy.wait_recv()
            total = total + stage[s + 1][t][j]
        if s == 2:
            rows = slice(4 * matrix[t], 4 * matrix[t] + 4)
            out_ref[rows, (t % 2) * 128 : (t % 2 + 1) * 128] = total[:4]
            out_ref[rows, half + (t % 2) * 128 : half + (t % 2 + 1) * 128] = total[4:]
            return
        kept = keep[s][t]
        kept[...] = total
        buf = (kept, "".join(d for d in dims if d not in GONE[dim]))
        held[t] = (buf, exchange_start(t, s + 1, buf, pick_part, place, device_of, send, stage))

    acc[1] += nt(owned[...], um[...])
    symmetrize(1)
    swap(0)
    swap(1)
    for stiff in later:
        stiff()
    acc[0] = nt(owned[...], us[...])
    acc[0] += nt(ht[...], hfar[...])
    for pair in range(pairs):
        acc[0] += nt(vt[pair], ys[pair])
        if pair == 1:
            swapped(0)
            swapped(1)
    symmetrize(0)
    swap(2)
    swap(3)
    swapped(2)
    swapped(3)
    for s in range(3):
        for t in range(tiles):
            advance(t, s)
    for copy in pending:
        copy.wait_send()
    for k, link in enumerate(links):
        @pl.when(sends_if(link))
        def _(k=k):
            for copy in copies[k]:
                copy.wait_send()


def local_sums(eigvecs, material):
    nx, ny, nz, cols = eigvecs.shape
    n = ny * nz
    count = {a: lax.axis_size(a) for a in ("gx", "gy", "gz")}
    cells = nx * ny * nz * count["gx"] * count["gy"] * count["gz"]
    plane, wy, wz = (jnp.asarray(w, BF16) for w in weight_arrays(nx, ny, nz))
    width = nx * nz
    shapes, keeps = stage_shapes()
    own_cells = 3 * n + nx * ny
    halo_cells = 2 * (32 + (nx // 2 + 2) * nz) + n + (ny + 8) * nx
    anyspace = pl.BlockSpec(memory_space=pl.ANY)
    vmem = pl.BlockSpec(memory_space=pltpu.VMEM)
    kernel = lambda *refs: local_kernel(
        (nx, ny, nz, cols, count["gx"], count["gy"]), 0.5 / cells, *refs
    )
    return pl.pallas_call(
        kernel,
        out_shape=pltpu.VMEM((8, cols), F32),
        in_specs=[anyspace, vmem] + [anyspace] * 3,
        out_specs=vmem,
        scratch_shapes=[
            pltpu.VMEM((nx, ny, nz, cols), BF16),
            pltpu.VMEM((nx // 2, cols, 2 * n), BF16),
            pltpu.VMEM((6, cols, 2 * n), F32),
            pltpu.VMEM((2, cols, 2 * n), BF16),
            pltpu.VMEM((2, cols, cols), F32),
            pltpu.VMEM((nx // 2 + 2, nz, cols), BF16),
            pltpu.VMEM((ny, nz, cols), BF16),
            pltpu.VMEM((ny + 8, nx, cols), BF16),
            pltpu.VMEM((5, 8, width), F32),
            pltpu.SemaphoreType.DMA((nx,)),
            pltpu.SemaphoreType.DMA((29,)),
            pltpu.SemaphoreType.DMA((29,)),
            pltpu.VMEM((2, 2, 2, 4, 4, 2, 8, cols // 2), F32),
            pltpu.SemaphoreType.DMA((10 * tiles,)),
            pltpu.SemaphoreType.DMA((10 * tiles,)),
            pltpu.VMEM((8, width), F32),
            pltpu.VMEM((ny, nx, cols), BF16),
            pltpu.VMEM((2, nx, cols), BF16),
            pltpu.VMEM(plane.shape, BF16),
            pltpu.VMEM(wy.shape, BF16),
            pltpu.VMEM(wz.shape, BF16),
            pltpu.SemaphoreType.DMA((3,)),
            pltpu.VMEM((nx // 2, cols, 2 * n), BF16),
            pltpu.VMEM((cols, halo_cells), BF16),
            pltpu.VMEM((cols, halo_cells), BF16),
        ]
        + [pltpu.VMEM((cols, own_cells), BF16)] * 3
        + [pltpu.VMEM((nx // 2, nz, cols), BF16), pltpu.VMEM((nz, cols), BF16)]
        + [pltpu.VMEM((2, nx, cols), BF16), pltpu.VMEM((8, 256), F32), pltpu.VMEM((9, 8, 256), F32)]
        + [pltpu.VMEM(x, F32) for row in shapes + keeps for x in row],
        compiler_params=pltpu.CompilerParams(
            collective_id=0, has_side_effects=True, vmem_limit_bytes=63 * 1024 * 1024
        ),
        name="local_sums",
    )(eigvecs, material, plane, wy, wz)


def per_device(eigvecs, material):
    both = local_sums(eigvecs, material)
    return both[:4], both[4:]


def solution(mesh):
    return jax.shard_map(
        per_device,
        mesh=mesh,
        in_specs=(P("gx", "gy", "gz", None), P(None, "gx", "gy", "gz")),
        out_specs=(P(("gx", "gy", "gz"), None), P(("gx", "gy", "gz"), None)),
        check_vma=False,
    )
```

```python
import jax
import jax.numpy as jnp
import numpy as np
from jax import lax
from jax.experimental import pallas as pl
from jax.experimental.pallas import tpu as pltpu
from jax.sharding import PartitionSpec as P

MESH = pl.DeviceIdType.MESH
F32, BF16 = jnp.float32, jnp.bfloat16
PC, PM = 1.0 / 16.0, 1.0 / 216.0


def taps(rows, cols, middle):
    gap = np.abs(rows[:, None] - cols[None, :])
    return np.where(gap == 0, middle, np.where(gap == 1, 1, 0))


def pair_weights(halo, own, middle):
    total = 1
    for h, o in zip(halo, own):
        total = total * taps(h, o, middle)
    return total


def grid(*axes):
    return [a.reshape(-1) for a in np.meshgrid(*axes, indexing="ij")]


def stacked(halo, own, pad):
    w = np.concatenate([pair_weights(halo, own, 2), pair_weights(halo, own, 4)], axis=1)
    w = np.concatenate([w, np.zeros((pad, w.shape[1]), w.dtype)], axis=0)
    return w.astype(np.float32)


WINDOWS = ((0, 256), (0, 384), (128, 384))
YWINDOWS = ((0, 256), (128, 384), (256, 512))
ZWINDOWS = ((0, 256),)


RELAY = 5
EARLY = 4


def banded(w, windows):
    m = w.shape[1] // 2
    found = []
    for t, (lo, hi) in enumerate(windows):
        own = np.r_[t * 128 : (t + 1) * 128, m + t * 128 : m + (t + 1) * 128]
        outside = np.delete(w[:, own], np.s_[lo:hi], axis=0)
        assert not outside.any()
        found.append(w[lo:hi][:, own])
    return np.concatenate(found)


def weight_arrays(nx, ny, nz):
    hx = nx // 2
    y, z = grid(np.arange(ny), np.arange(nz))
    plane = banded(stacked([y, z], [y, z], 0), WINDOWS)
    hxx, hzz = grid(np.arange(-1, hx + 1), np.arange(nz))
    oxx, ozz = grid(np.arange(hx), np.arange(nz))
    wy = stacked([hxx, hzz, 0 * hxx + 1], [oxx, ozz, 0 * oxx], 16)
    wy = banded(np.concatenate([np.zeros((16, wy.shape[1]), np.float32), wy]), YWINDOWS)
    far = 99
    slabs = []
    xs = np.arange(nx)
    for yy in range(ny):
        slabs.append((xs, 0 * xs + yy))
    ys = np.concatenate([np.arange(ny), far + 0 * np.arange(nx - ny)])
    first = np.where(xs == 0, 0, far)
    last = np.where(xs == nx - 1, 0, far)
    slabs += [(xs, 0 * xs - 1), (xs, 0 * xs + ny)]
    slabs += [(0 * xs - 1, ys), (0 * xs + nx, ys)]
    slabs += [(last - 1, 0 * xs - 1), (last - 1, 0 * xs + ny)]
    slabs += [(first + nx, 0 * xs - 1), (first + nx, 0 * xs + ny)]
    zx = np.concatenate([s[0] for s in slabs])
    zy = np.concatenate([s[1] for s in slabs])
    oyy, oxx = grid(np.arange(ny), np.arange(nx))
    wz = banded(stacked([zx, zy, 0 * zx + 1], [oxx, oyy, 0 * oxx], 0), ZWINDOWS)
    return plane, wy, wz


def nt(a, b):
    return lax.dot_general(a, b, (((1,), (1,)), ((), ())), preferred_element_type=F32)


def nn(a, b):
    return jnp.dot(a, b, preferred_element_type=F32)


def split(x):
    pad = jnp.zeros(((-x.shape[0]) % 16, x.shape[1]), F32)
    x = jnp.concatenate([x, pad], axis=0) if pad.shape[0] else x
    high = x.astype(BF16)
    rest = x - high.astype(F32)
    mid = rest.astype(BF16)
    low = (rest - mid.astype(F32)).astype(BF16)
    return jnp.concatenate([high, mid, low], axis=0)


def joined(x, rows):
    return (x[:rows] + x[16 : 16 + rows]) + x[32 : 32 + rows]


def exact(a, b):
    return joined(nn(split(a), b), a.shape[0])


def exact_nt(a, b):
    return joined(nt(split(a), b), a.shape[0])


ORDERS = ("yxz", "xzy", "zyx", "xyz")
GONE = {"x": "x", "y": "y", "z": "lh"}
SIZE = {"l": 2, "h": 2, "x": 4, "y": 4}
tiles = len(ORDERS)


def exchange_start(t, s, held, pick, place, device_of, send, stage):
    buf, dims = held
    dim = ORDERS[t][s]
    copies = []
    for j in range(3):
        at = lax.rem(place[dim] + j + 1, 4)
        copies.append(
            send(
                buf.at[pick(buf, dims, dim, at)], stage[s + 1][t].at[j],
                tiles + (s * tiles + t) * 3 + j, device_of(dim, at),
            )
        )
    return copies


def partners(gx, gy, gz):
    core, z = lax.rem(gx, 2), gz * 2 + gx // 2
    x, y = gy // 4, lax.rem(gy, 4)
    found = [(gx + 1 - 2 * core, gy, gz)]
    for j in range(1, 4):
        found.append((gx, x * 4 + lax.rem(y + j, 4), gz))
        found.append((gx, lax.rem(x + j, 4) * 4 + y, gz))
        zz = lax.rem(z + j, 4)
        found.append((lax.rem(zz, 2) * 2 + core, gy, zz // 2))
    return found


def stage_shapes():
    shapes, keeps = [[(2, 4, 4, 2, 8, 128)] * tiles], []
    for s in range(3):
        row, kept = [], []
        for t in range(tiles):
            gone = "".join(GONE[d] for d in ORDERS[t][: s + 1])
            left = tuple(SIZE[d] for d in "lxyh" if d not in gone) + (8, 128)
            row.append((3,) + left)
            kept.append(left)
        shapes.append(row)
        keeps.append(kept)
    return shapes, keeps[:2]


def local_kernel(
    dims, scale,
    v_ref, mat_ref, wp_any, wy_any, wz_any,
    out_ref,
    vbuf, vt, fbuf, ym, acc, hy, hx, hz, fh, vsem, send_sem, recv_sem,
    q, rsend, rrecv, faces_ref, zf_ref, zx_ref, wp_ref, wy_ref, wz_ref, wsem,
    ys, ht, hfar, owned, us, um, hu, hc, hzx, fz_ref, fhz, *rest,
):
    stage = [rest[s * tiles : (s + 1) * tiles] for s in range(4)]
    keep = [rest[(4 + s) * tiles : (5 + s) * tiles] for s in range(2)]
    nx, ny, nz, cols, ngx, ngy = dims
    n = ny * nz
    gx, gy, gz = lax.axis_index("gx"), lax.axis_index("gy"), lax.axis_index("gz")
    hx_n = nx // 2

    loads = [pltpu.make_async_copy(v_ref.at[x], vbuf.at[x], vsem.at[x]) for x in range(nx)]
    weights = [
        pltpu.make_async_copy(a, b, wsem.at[k])
        for k, (a, b) in enumerate(((wp_any, wp_ref), (wy_any, wy_ref), (wz_any, wz_ref)))
    ]
    weights[0].start()
    for load in loads:
        load.start()
    for load in weights[1:]:
        load.start()

    links = [
        ((0, 1), 0, v_ref.at[pl.ds(0, hx_n + 1), ny - 1], hy.at[pl.ds(1, hx_n + 1)]),
        ((1, 1), 0, v_ref.at[nx - 1, ny - 1], hy.at[0]),
        ((-1, 0), 0, v_ref.at[0, ny - 1], hc),
        ((1, 0), 0, v_ref.at[nx - 1], hx),
        ((0, -1), 0, v_ref.at[pl.ds(hx_n, hx_n), 0], hu),
    ]
    links = [(o, kind, [(faces_ref, fh.at[k]), (a, b)]) for k, (o, kind, a, b) in enumerate(links)]
    cut = ((0, 0), 1, [(fz_ref, fhz.at[0]), (zf_ref, hz.at[pl.ds(0, ny)]), (zx_ref, hzx)])
    relays = [
        ((0, 1), hz.at[ny - 1]), ((0, -1), hz.at[0]), ((1, 0), hzx.at[1]), ((-1, 0), hzx.at[0]),
        ((1, 1), hz.at[ny - 1]), ((1, -1), hz.at[0]), ((-1, 1), hz.at[ny - 1]), ((-1, -1), hz.at[0]),
    ]
    links = links + [cut] + [
        (o, 2, [(fhz.at[0], fhz.at[j + 1]), (a, hz.at[ny + j])]) for j, (o, a) in enumerate(relays)
    ]

    def inside(dx, dy):
        ok = None
        for move, at, count in ((dx, gx, ngx), (dy, gy, ngy)):
            here = None
            if move == 1:
                here = at < count - 1
            if move == -1:
                here = at > 0
            if here is not None:
                ok = here if ok is None else jnp.logical_and(ok, here)
        return ok

    def both(a, b):
        return b if a is None else jnp.logical_and(a, b)

    def sends_if(link):
        (dx, dy), kind, _ = link
        ok = inside(dx, dy)
        return both(ok, gz == kind - 1) if kind else ok

    def gets_if(link):
        (dx, dy), kind, _ = link
        ok = inside(-dx, -dy)
        return both(ok, gz == 1) if kind else ok

    hy[...] = jnp.zeros_like(hy)
    hx[...] = jnp.zeros_like(hx)
    hu[...] = jnp.zeros_like(hu)
    hc[...] = jnp.zeros_like(hc)
    hz[...] = jnp.zeros_like(hz)
    hzx[...] = jnp.zeros_like(hzx)
    fh[...] = jnp.zeros_like(fh)
    fhz[...] = jnp.zeros_like(fhz)

    barrier = pltpu.get_barrier_semaphore()
    targets = 0
    for link in links:
        (dx, dy), kind, _ = link
        source = (gx - dx, gy - dy, 0 if kind == 1 else gz)

        @pl.when(gets_if(link))
        def _(source=source):
            pl.semaphore_signal(barrier, inc=1, device_id=source, device_id_type=MESH)

        targets = targets + sends_if(link).astype(jnp.int32)
    for device in partners(gx, gy, gz):
        pl.semaphore_signal(barrier, inc=1, device_id=device, device_id_type=MESH)

    copies = []
    used_sems = 0
    for (dx, dy), kind, moves in links:
        device = (gx + dx, gy + dy, 1 if kind == 1 else gz)
        group_of = []
        for a, b in moves:
            group_of.append(
                pltpu.make_async_remote_copy(
                    src_ref=a, dst_ref=b, send_sem=send_sem.at[used_sems],
                    recv_sem=recv_sem.at[used_sems], device_id=device, device_id_type=MESH,
                )
            )
            used_sems += 1
        copies.append(group_of)

    def wait_if(link, k):
        @pl.when(gets_if(link))
        def _():
            for copy in copies[k]:
                copy.wait_recv()

    def relay():
        wait_if(cut, links.index(cut))
        for link, pair in zip(links, copies):
            if link[1] == 2:

                @pl.when(sends_if(link))
                def _(pair=pair):
                    for copy in pair:
                        copy.start()

    def first_sends():
        pl.semaphore_wait(barrier, targets + 10)
        for link, pair in zip(links, copies):
            if link[1] == 0:

                @pl.when(sends_if(link))
                def _(pair=pair):
                    pair[1].start()

    first_sends()
    kappa, rho = (
        jnp.concatenate([mat_ref[j, :, y, :] for y in range(ny)], axis=1) for j in range(2)
    )
    at_low = gz == 1
    cell = lax.broadcasted_iota(jnp.int32, (n, 128), 0)
    lane = lax.broadcasted_iota(jnp.int32, (n, 128), 1)
    edge_z = jnp.where(at_low, 0, nz - 1)
    hot = jnp.logical_and(cell == lane * nz + edge_z, lane < ny).astype(F32).astype(BF16)
    width = nx * nz
    for j, rows in enumerate((kappa, rho)):
        faces_ref[j : j + 1, :] = jnp.concatenate(
            [rows[x : x + 1, (ny - 1) * nz :] for x in range(nx)], axis=1
        )
        faces_ref[4 + j : 5 + j, :] = jnp.concatenate(
            [rows[x : x + 1, :nz] for x in range(nx)], axis=1
        )
        faces_ref[2 + j : 3 + j, :] = jnp.concatenate(
            [rows[nx - 1 :], jnp.zeros((1, width - n), F32)], axis=1
        )
        edge_rows = exact(rows, hot)
        turned = jnp.concatenate([edge_rows, jnp.zeros((128 - nx, 128), F32)], axis=0).T
        fz_ref[j : j + 1, :] = jnp.concatenate(
            [turned[y : y + 1, :nx] for y in range(ny)]
            + [edge_rows[:1, :nx], edge_rows[nx - 1 :, :nx]]
            + [jnp.zeros((1, 256 - (ny + 2) * nx), F32)],
            axis=1,
        )

    faces_ref[6:, :] = jnp.zeros((2, width), F32)
    fz_ref[2:, :] = jnp.zeros((6, 256), F32)

    def z_edge(x, y, count):
        tall, low = vbuf[x, y, nz - 16 :, :], vbuf[x, y, :16, :]
        picked = jnp.where(at_low, low.astype(F32)[:, 0, :], tall.astype(F32)[:, 15, :])
        return picked.astype(BF16)

    def later_sends():
        for load in loads[5:]:
            load.wait()
        for y in range(ny):
            zf_ref[y] = z_edge(slice(None), y, nx)
        zx_ref[...] = jnp.zeros_like(zx_ref)
        for j, x in enumerate((0, nx - 1)):
            zx_ref[j, :ny] = z_edge(x, slice(None), ny)
        for link, pair in zip(links, copies):

            if link[1] < 2:

                @pl.when(sends_if(link))
                def _(link=link, pair=pair):
                    for copy in pair if link[1] else pair[:1]:
                        copy.start()

    weights[0].wait()
    starts = np.cumsum([0] + [hi - lo for lo, hi in WINDOWS])
    zero = jnp.zeros((1, n), F32)
    filtered = jnp.concatenate(
        [
            exact(kappa[:, lo:hi], wp_ref[starts[t] : starts[t + 1], :128])
            for t, (lo, hi) in enumerate(WINDOWS)
        ],
        axis=1,
    )
    around = (
        jnp.concatenate([zero, filtered[:-1]], axis=0)
        + 2.0 * filtered
        + jnp.concatenate([filtered[1:], zero], axis=0)
    )
    diag = 0.5 * (3.5 * kappa + PC * around - 0.5 * kappa)
    coef_v = diag + 0.5 * kappa
    coef_s = PC * kappa
    coef_m = PM * rho

    def load_plane(x):
        if x < nx:
            if x < 5:
                loads[x].wait()
            vt[x // 2, :, (x % 2) * n : (x % 2 + 1) * n] = vbuf[x].reshape(n, cols).T

    def stage_a(x):
        if x < nx:
            load_plane(x)
            for t, (lo, hi) in enumerate(WINDOWS):
                base = (x % 2) * n
                fbuf[x % 6, :, t * 256 : (t + 1) * 256] = nn(
                    vt[x // 2, :, base + lo : base + hi], wp_ref[starts[t] : starts[t + 1]]
                )

    chunk = 32

    def stage_b(x, lo, hi):
        half = (x % 2) * n
        buf = (x // 2) % 2
        for r in range(lo, hi, chunk):
            rows = slice(r, r + chunk)
            for t in range(n // 128):
                cv, cs, cm = (
                    c[x : x + 1, t * 128 : (t + 1) * 128] for c in (coef_v, coef_s, coef_m)
                )
                at_s = slice(t * 256, t * 256 + 128)
                at_m = slice(t * 256 + 128, (t + 1) * 256)
                at_v = slice(half + t * 128, half + (t + 1) * 128)
                s = 2.0 * fbuf[x % 6, rows, at_s]
                m = 4.0 * fbuf[x % 6, rows, at_m]
                for near in (x - 1, x + 1):
                    if 0 <= near < nx:
                        s = s + fbuf[near % 6, rows, at_s]
                        m = m + fbuf[near % 6, rows, at_m]
                v = vt[x // 2, rows, at_v].astype(F32)
                ys[x // 2, rows, at_v] = (cv * v - cs * s).astype(BF16)
                ym[buf, rows, at_v] = (cm * m).astype(BF16)

    def stage_c(pair):
        if pair < 0:
            return
        part = nt(vt[pair], ym[pair % 2])
        if pair == 0:
            acc[1] = part
        else:
            acc[1] += part

    pairs = nx // 2
    for x in range(3):
        stage_a(x)
    for i in range(pairs):
        for x in range(2):
            stage_a(2 * i + 3 + x)
            stage_b(2 * i + x, 0, cols)
        stage_c(i - 1)
        if i == 0:
            later_sends()
        if i == RELAY:
            relay()
    stage_c(pairs - 1)
    for load in weights[1:]:
        load.wait()

    def wait_for(*ks):
        for k in ks:
            wait_if(links[k], k)

    def row(k, r, lo, hi):
        return fh[k, r : r + 1, lo:hi]

    def wide(x):
        return jnp.concatenate(x, axis=1)

    used = (hx_n + 2) * nz
    blank = jnp.zeros((1, 16), F32)
    edge = (nx - 1) * nz

    later = []

    def group(k_at, m_at, halo, kh, rh, own, ko, ro, w_ref, windows):
        k, m = halo.shape[0], own.shape[1]
        ht[:, k_at : k_at + k] = halo.T
        owned[:, m_at : m_at + m] = own
        rc = jnp.broadcast_to(rh, (128, k)).T
        spans = np.cumsum([0] + [hi - lo for lo, hi in windows])
        for t, (lo, hi) in enumerate(windows):
            lanes = slice(t * 128, (t + 1) * 128)
            wm = w_ref[spans[t] : spans[t + 1], 128:].astype(F32)
            lm = (wm * (PM * (rc[lo:hi] + ro[:, lanes]))).astype(BF16)
            at = slice(m_at + t * 128, m_at + (t + 1) * 128)
            um[:, at] = nn(ht[:, k_at + lo : k_at + hi], lm).astype(BF16)

        def stiff():
            kc = jnp.broadcast_to(kh, (128, k)).T
            far = jnp.zeros((1, k), F32)
            for t, (lo, hi) in enumerate(windows):
                lanes = slice(t * 128, (t + 1) * 128)
                tile = w_ref[spans[t] : spans[t + 1], :128]
                wc = tile.astype(F32)
                ls = (wc * ((-PC) * (kc[lo:hi] + ko[:, lanes]))).astype(BF16)
                fbuf[t, :, :128] = nn(ht[:, k_at + lo : k_at + hi], ls)
                own_diag = (0.5 * PC) * jnp.sum(wc * kc[lo:hi], axis=0, keepdims=True)
                part = (0.5 * PC) * exact_nt(ko[:, lanes], tile)
                sides = [jnp.zeros((1, lo), F32), part, jnp.zeros((1, k - hi), F32)]
                far = far + wide([x for x in sides if x.shape[1]])
                at = slice(m_at + t * 128, m_at + (t + 1) * 128)
                for r in range(0, cols, 64):
                    rows = slice(r, r + 64)
                    us[rows, at] = (
                        own_diag * owned[rows, at].astype(F32) + fbuf[t, rows, :128]
                    ).astype(BF16)
            for r in range(0, cols, 32):
                rows = slice(r, r + 32)
                at = slice(k_at, k_at + k)
                hfar[rows, at] = (far * ht[rows, at].astype(F32)).astype(BF16)

        later.append(stiff)

    ky = 2 * 16 + used
    acc[0] = nt(vt[0], ys[0])
    for pair in range(1, EARLY):
        acc[0] += nt(vt[pair], ys[pair])
    wait_for(3)
    group(
        2 * ky, 2 * n, hx[...].reshape(n, cols), row(3, 2, 0, n), row(3, 3, 0, n),
        vt[0, :, :n], kappa[:1], rho[:1], wp_ref, WINDOWS,
    )

    wait_for(*range(6, 14))
    nf = nx * ny
    low, high = (nf - nx, nf), (0, nx)

    def zpick(r):
        spans = [(0, nf), low, high, (nf + nx, nf + 2 * nx), (nf, nf + nx), low, high, low, high]
        return wide([fhz[k, r : r + 1, lo:hi] for k, (lo, hi) in enumerate(spans)])

    group(
        2 * ky + n, 3 * n, hz[...].reshape((ny + 8) * nx, cols), zpick(0), zpick(1),
        zf_ref[...].reshape(nf, cols).T, fz_ref[:1, :nf], fz_ref[1:2, :nf],
        wz_ref, ZWINDOWS,
    )

    wait_for(0, 1)
    none = jnp.zeros((16, cols), BF16)
    lower = lambda r: wide([blank, row(1, r, edge, edge + nz), row(0, r, 0, used - nz), blank])
    group(
        0, 0, jnp.concatenate([none, hy[...].reshape(used, cols), none], axis=0),
        lower(0), lower(1), vbuf[:hx_n, 0].reshape(hx_n * nz, cols).T,
        *(wide([rows[x : x + 1, :nz] for x in range(hx_n)]) for rows in (kappa, rho)),
        wy_ref, YWINDOWS,
    )
    wait_for(2, 4)
    upper = lambda r: wide(
        [blank, faces_ref[r : r + 1, (hx_n - 1) * nz :], row(2, r, 0, nz), blank]
    )
    mine = vbuf[hx_n - 1 :, ny - 1].reshape(used - nz, cols)
    group(
        ky, n, jnp.concatenate([none, mine, hc[...], none], axis=0),
        upper(0), upper(1), hu[...].reshape(hx_n * nz, cols).T,
        row(4, 4, hx_n * nz, nx * nz), row(4, 5, hx_n * nz, nx * nz), wy_ref, YWINDOWS,
    )

    core, zl = lax.rem(gx, 2), gx // 2
    place = {"x": gy // 4, "y": lax.rem(gy, 4), "z": gz * 2 + zl}

    def device_of(dim, at):
        x, y, z = (at if dim == d else place[d] for d in "xyz")
        return (lax.rem(z, 2) * 2 + core, x * 4 + y, z // 2)

    pending = []

    def send(source, target, sem, device):
        copy = pltpu.make_async_remote_copy(
            src_ref=source, dst_ref=target, send_sem=rsend.at[sem], recv_sem=rrecv.at[sem],
            device_id=device, device_id_type=MESH,
        )
        copy.start()
        pending.append(copy)
        return copy

    def pick_part(buf, dims, dim, at):
        index = []
        for d in dims:
            hit = {"l": lax.rem(at, 2), "h": at // 2}.get(d) if dim == "z" else at if d == dim else None
            index.append(slice(None) if hit is None else hit)
        return tuple(index)

    half = cols // 2
    low_rows = lax.broadcasted_iota(jnp.int32, (16, 8, half), 1) < 4

    def symmetrize(h):
        for b in range(4):
            block = slice(b * 128, (b + 1) * 128)
            total = (acc[h, block] + acc[h, :, block].T) * scale
            left, right = total[:, :half].reshape(16, 8, half), total[:, half:].reshape(16, 8, half)
            first = jnp.where(low_rows, left, pltpu.roll(right, 4, 1))
            second = jnp.where(low_rows, pltpu.roll(left, 4, 1), right)
            q[h, b // 2, b % 2, :, :, 0] = first.reshape(4, 4, 8, half)
            q[h, b // 2, b % 2, :, :, 1] = second.reshape(4, 4, 8, half)

    matrix = (1, 1, 0, 0)
    held = [None] * tiles

    def swap(t):
        lanes = slice((t % 2) * 128, (t % 2 + 1) * 128)
        held[t] = send(
            q.at[matrix[t], :, 1 - core, :, :, :, :, lanes], stage[0][t], t,
            (zl * 2 + 1 - core, gy, gz),
        )

    def swapped(t):
        lanes = slice((t % 2) * 128, (t % 2 + 1) * 128)
        held[t].wait_recv()
        stage[0][t][...] += q[matrix[t], :, core, :, :, :, :, lanes]
        buf = (stage[0][t], "lxyh")
        held[t] = (buf, exchange_start(t, 0, buf, pick_part, place, device_of, send, stage))

    def advance(t, s):
        (buf, dims), copies_t = held[t]
        dim = ORDERS[t][s]
        total = buf[pick_part(buf, dims, dim, place[dim])]
        for j, copy in enumerate(copies_t):
            copy.wait_recv()
            total = total + stage[s + 1][t][j]
        if s == 2:
            rows = slice(4 * matrix[t], 4 * matrix[t] + 4)
            out_ref[rows, (t % 2) * 128 : (t % 2 + 1) * 128] = total[:4]
            out_ref[rows, half + (t % 2) * 128 : half + (t % 2 + 1) * 128] = total[4:]
            return
        kept = keep[s][t]
        kept[...] = total
        buf = (kept, "".join(d for d in dims if d not in GONE[dim]))
        held[t] = (buf, exchange_start(t, s + 1, buf, pick_part, place, device_of, send, stage))

    acc[1] += nt(owned[...], um[...])
    symmetrize(1)
    swap(0)
    swap(1)
    for stiff in later:
        stiff()
    acc[0] += nt(owned[...], us[...])
    acc[0] += nt(ht[...], hfar[...])
    for pair in range(EARLY, pairs):
        acc[0] += nt(vt[pair], ys[pair])
        if pair == 6:
            swapped(0)
            swapped(1)
    symmetrize(0)
    swap(2)
    swap(3)
    swapped(2)
    swapped(3)
    for s in range(3):
        for t in range(tiles):
            advance(t, s)
    for copy in pending:
        copy.wait_send()
    for k, link in enumerate(links):
        @pl.when(sends_if(link))
        def _(k=k):
            for copy in copies[k]:
                copy.wait_send()


def local_sums(eigvecs, material):
    nx, ny, nz, cols = eigvecs.shape
    n = ny * nz
    count = {a: lax.axis_size(a) for a in ("gx", "gy", "gz")}
    cells = nx * ny * nz * count["gx"] * count["gy"] * count["gz"]
    plane, wy, wz = (jnp.asarray(w, BF16) for w in weight_arrays(nx, ny, nz))
    width = nx * nz
    shapes, keeps = stage_shapes()
    own_cells = 3 * n + nx * ny
    halo_cells = 2 * (32 + (nx // 2 + 2) * nz) + n + (ny + 8) * nx
    anyspace = pl.BlockSpec(memory_space=pl.ANY)
    vmem = pl.BlockSpec(memory_space=pltpu.VMEM)
    kernel = lambda *refs: local_kernel(
        (nx, ny, nz, cols, count["gx"], count["gy"]), 0.5 / cells, *refs
    )
    return pl.pallas_call(
        kernel,
        out_shape=pltpu.VMEM((8, cols), F32),
        in_specs=[anyspace, vmem] + [anyspace] * 3,
        out_specs=vmem,
        scratch_shapes=[
            pltpu.VMEM((nx, ny, nz, cols), BF16),
            pltpu.VMEM((nx // 2, cols, 2 * n), BF16),
            pltpu.VMEM((6, cols, 2 * n), F32),
            pltpu.VMEM((2, cols, 2 * n), BF16),
            pltpu.VMEM((2, cols, cols), F32),
            pltpu.VMEM((nx // 2 + 2, nz, cols), BF16),
            pltpu.VMEM((ny, nz, cols), BF16),
            pltpu.VMEM((ny + 8, nx, cols), BF16),
            pltpu.VMEM((5, 8, width), F32),
            pltpu.SemaphoreType.DMA((nx,)),
            pltpu.SemaphoreType.DMA((29,)),
            pltpu.SemaphoreType.DMA((29,)),
            pltpu.VMEM((2, 2, 2, 4, 4, 2, 8, cols // 2), F32),
            pltpu.SemaphoreType.DMA((10 * tiles,)),
            pltpu.SemaphoreType.DMA((10 * tiles,)),
            pltpu.VMEM((8, width), F32),
            pltpu.VMEM((ny, nx, cols), BF16),
            pltpu.VMEM((2, nx, cols), BF16),
            pltpu.VMEM(plane.shape, BF16),
            pltpu.VMEM(wy.shape, BF16),
            pltpu.VMEM(wz.shape, BF16),
            pltpu.SemaphoreType.DMA((3,)),
            pltpu.VMEM((nx // 2, cols, 2 * n), BF16),
            pltpu.VMEM((cols, halo_cells), BF16),
            pltpu.VMEM((cols, halo_cells), BF16),
        ]
        + [pltpu.VMEM((cols, own_cells), BF16)] * 3
        + [pltpu.VMEM((nx // 2, nz, cols), BF16), pltpu.VMEM((nz, cols), BF16)]
        + [pltpu.VMEM((2, nx, cols), BF16), pltpu.VMEM((8, 256), F32), pltpu.VMEM((9, 8, 256), F32)]
        + [pltpu.VMEM(x, F32) for row in shapes + keeps for x in row],
        compiler_params=pltpu.CompilerParams(
            collective_id=0, has_side_effects=True, vmem_limit_bytes=63 * 1024 * 1024
        ),
        name="local_sums",
    )(eigvecs, material, plane, wy, wz)


def per_device(eigvecs, material):
    both = local_sums(eigvecs, material)
    return both[:4], both[4:]


def solution(mesh):
    return jax.shard_map(
        per_device,
        mesh=mesh,
        in_specs=(P("gx", "gy", "gz", None), P(None, "gx", "gy", "gz")),
        out_specs=(P(("gx", "gy", "gz"), None), P(("gx", "gy", "gz"), None)),
        check_vma=False,
    )
```

```python
import jax
import jax.numpy as jnp
import numpy as np
from jax import lax
from jax.experimental import pallas as pl
from jax.experimental.pallas import tpu as pltpu
from jax.sharding import PartitionSpec as P

MESH = pl.DeviceIdType.MESH
F32, BF16 = jnp.float32, jnp.bfloat16
PC, PM = 1.0 / 16.0, 1.0 / 216.0


def taps(rows, cols, middle):
    gap = np.abs(rows[:, None] - cols[None, :])
    return np.where(gap == 0, middle, np.where(gap == 1, 1, 0))


def pair_weights(halo, own, middle):
    total = 1
    for h, o in zip(halo, own):
        total = total * taps(h, o, middle)
    return total


def grid(*axes):
    return [a.reshape(-1) for a in np.meshgrid(*axes, indexing="ij")]


def stacked(halo, own, pad):
    w = np.concatenate([pair_weights(halo, own, 2), pair_weights(halo, own, 4)], axis=1)
    w = np.concatenate([w, np.zeros((pad, w.shape[1]), w.dtype)], axis=0)
    return w.astype(np.float32)


WINDOWS = ((0, 256), (0, 384), (128, 384))
YWINDOWS = ((0, 256), (128, 384), (256, 512))
ZWINDOWS = ((0, 256),)


RELAY = 5
EARLY = 4


def banded(w, windows):
    m = w.shape[1] // 2
    found = []
    for t, (lo, hi) in enumerate(windows):
        own = np.r_[t * 128 : (t + 1) * 128, m + t * 128 : m + (t + 1) * 128]
        outside = np.delete(w[:, own], np.s_[lo:hi], axis=0)
        assert not outside.any()
        found.append(w[lo:hi][:, own])
    return np.concatenate(found)


def weight_arrays(nx, ny, nz):
    hx = nx // 2
    y, z = grid(np.arange(ny), np.arange(nz))
    plane = banded(stacked([y, z], [y, z], 0), WINDOWS)
    hxx, hzz = grid(np.arange(-1, hx + 1), np.arange(nz))
    oxx, ozz = grid(np.arange(hx), np.arange(nz))
    wy = stacked([hxx, hzz, 0 * hxx + 1], [oxx, ozz, 0 * oxx], 16)
    wy = banded(np.concatenate([np.zeros((16, wy.shape[1]), np.float32), wy]), YWINDOWS)
    far = 99
    slabs = []
    xs = np.arange(nx)
    for yy in range(ny):
        slabs.append((xs, 0 * xs + yy))
    ys = np.concatenate([np.arange(ny), far + 0 * np.arange(nx - ny)])
    first = np.where(xs == 0, 0, far)
    last = np.where(xs == nx - 1, 0, far)
    slabs += [(xs, 0 * xs - 1), (xs, 0 * xs + ny)]
    slabs += [(0 * xs - 1, ys), (0 * xs + nx, ys)]
    slabs += [(last - 1, 0 * xs - 1), (last - 1, 0 * xs + ny)]
    slabs += [(first + nx, 0 * xs - 1), (first + nx, 0 * xs + ny)]
    zx = np.concatenate([s[0] for s in slabs])
    zy = np.concatenate([s[1] for s in slabs])
    oyy, oxx = grid(np.arange(ny), np.arange(nx))
    wz = banded(stacked([zx, zy, 0 * zx + 1], [oxx, oyy, 0 * oxx], 0), ZWINDOWS)
    return plane, wy, wz


def nt(a, b):
    return lax.dot_general(a, b, (((1,), (1,)), ((), ())), preferred_element_type=F32)


def nn(a, b):
    return jnp.dot(a, b, preferred_element_type=F32)


def split(x):
    pad = jnp.zeros(((-x.shape[0]) % 16, x.shape[1]), F32)
    x = jnp.concatenate([x, pad], axis=0) if pad.shape[0] else x
    high = x.astype(BF16)
    rest = x - high.astype(F32)
    mid = rest.astype(BF16)
    low = (rest - mid.astype(F32)).astype(BF16)
    return jnp.concatenate([high, mid, low], axis=0)


def joined(x, rows):
    return (x[:rows] + x[16 : 16 + rows]) + x[32 : 32 + rows]


def exact(a, b):
    return joined(nn(split(a), b), a.shape[0])


def exact_nt(a, b):
    return joined(nt(split(a), b), a.shape[0])


ORDERS = ("zyx", "zxy", "yxz", "xyz")
GONE = {"x": "x", "y": "y", "z": "lh"}
SIZE = {"l": 2, "h": 2, "x": 4, "y": 4}
tiles = len(ORDERS)


def exchange_start(t, s, held, pick, place, device_of, send, stage):
    buf, dims = held
    dim = ORDERS[t][s]
    copies = []
    for j in range(3):
        at = lax.rem(place[dim] + j + 1, 4)
        copies.append(
            send(
                buf.at[pick(buf, dims, dim, at)], stage[s + 1][t].at[j],
                tiles + (s * tiles + t) * 3 + j, device_of(dim, at),
            )
        )
    return copies


def partners(gx, gy, gz):
    core, z = lax.rem(gx, 2), gz * 2 + gx // 2
    x, y = gy // 4, lax.rem(gy, 4)
    found = [(gx + 1 - 2 * core, gy, gz)]
    for j in range(1, 4):
        found.append((gx, x * 4 + lax.rem(y + j, 4), gz))
        found.append((gx, lax.rem(x + j, 4) * 4 + y, gz))
        zz = lax.rem(z + j, 4)
        found.append((lax.rem(zz, 2) * 2 + core, gy, zz // 2))
    return found


def stage_shapes():
    shapes, keeps = [[(2, 4, 4, 2, 8, 128)] * tiles], []
    for s in range(3):
        row, kept = [], []
        for t in range(tiles):
            gone = "".join(GONE[d] for d in ORDERS[t][: s + 1])
            left = tuple(SIZE[d] for d in "lxyh" if d not in gone) + (8, 128)
            row.append((3,) + left)
            kept.append(left)
        shapes.append(row)
        keeps.append(kept)
    return shapes, keeps[:2]


def local_kernel(
    dims, scale,
    v_ref, mat_ref, wp_any, wy_any, wz_any,
    out_ref,
    vbuf, vt, fbuf, ym, acc, hy, hx, hz, fh, vsem, send_sem, recv_sem,
    q, rsend, rrecv, faces_ref, zf_ref, zx_ref, wp_ref, wy_ref, wz_ref, wsem,
    ys, ht, hfar, owned, us, um, hu, hc, hzx, fz_ref, fhz, *rest,
):
    stage = [rest[s * tiles : (s + 1) * tiles] for s in range(4)]
    keep = [rest[(4 + s) * tiles : (5 + s) * tiles] for s in range(2)]
    nx, ny, nz, cols, ngx, ngy = dims
    n = ny * nz
    gx, gy, gz = lax.axis_index("gx"), lax.axis_index("gy"), lax.axis_index("gz")
    hx_n = nx // 2

    loads = [pltpu.make_async_copy(v_ref.at[x], vbuf.at[x], vsem.at[x]) for x in range(nx)]
    weights = [
        pltpu.make_async_copy(a, b, wsem.at[k])
        for k, (a, b) in enumerate(((wp_any, wp_ref), (wy_any, wy_ref), (wz_any, wz_ref)))
    ]
    weights[0].start()
    for load in loads:
        load.start()
    for load in weights[1:]:
        load.start()

    links = [
        ((0, 1), 0, v_ref.at[pl.ds(0, hx_n + 1), ny - 1], hy.at[pl.ds(1, hx_n + 1)]),
        ((1, 1), 0, v_ref.at[nx - 1, ny - 1], hy.at[0]),
        ((-1, 0), 0, v_ref.at[0, ny - 1], hc),
        ((1, 0), 0, v_ref.at[nx - 1], hx),
        ((0, -1), 0, v_ref.at[pl.ds(hx_n, hx_n), 0], hu),
    ]
    links = [(o, kind, [(faces_ref, fh.at[k]), (a, b)]) for k, (o, kind, a, b) in enumerate(links)]
    cut = ((0, 0), 1, [(fz_ref, fhz.at[0]), (zf_ref, hz.at[pl.ds(0, ny)]), (zx_ref, hzx)])
    relays = [
        ((0, 1), hz.at[ny - 1]), ((0, -1), hz.at[0]), ((1, 0), hzx.at[1]), ((-1, 0), hzx.at[0]),
        ((1, 1), hz.at[ny - 1]), ((1, -1), hz.at[0]), ((-1, 1), hz.at[ny - 1]), ((-1, -1), hz.at[0]),
    ]
    links = links + [cut] + [
        (o, 2, [(fhz.at[0], fhz.at[j + 1]), (a, hz.at[ny + j])]) for j, (o, a) in enumerate(relays)
    ]

    def inside(dx, dy):
        ok = None
        for move, at, count in ((dx, gx, ngx), (dy, gy, ngy)):
            here = None
            if move == 1:
                here = at < count - 1
            if move == -1:
                here = at > 0
            if here is not None:
                ok = here if ok is None else jnp.logical_and(ok, here)
        return ok

    def both(a, b):
        return b if a is None else jnp.logical_and(a, b)

    def sends_if(link):
        (dx, dy), kind, _ = link
        ok = inside(dx, dy)
        return both(ok, gz == kind - 1) if kind else ok

    def gets_if(link):
        (dx, dy), kind, _ = link
        ok = inside(-dx, -dy)
        return both(ok, gz == 1) if kind else ok

    hy[...] = jnp.zeros_like(hy)
    hx[...] = jnp.zeros_like(hx)
    hu[...] = jnp.zeros_like(hu)
    hc[...] = jnp.zeros_like(hc)
    hz[...] = jnp.zeros_like(hz)
    hzx[...] = jnp.zeros_like(hzx)
    fh[...] = jnp.zeros_like(fh)
    fhz[...] = jnp.zeros_like(fhz)

    barrier = pltpu.get_barrier_semaphore()
    targets = 0
    for link in links:
        (dx, dy), kind, _ = link
        source = (gx - dx, gy - dy, 0 if kind == 1 else gz)

        @pl.when(gets_if(link))
        def _(source=source):
            pl.semaphore_signal(barrier, inc=1, device_id=source, device_id_type=MESH)

        targets = targets + sends_if(link).astype(jnp.int32)
    for device in partners(gx, gy, gz):
        pl.semaphore_signal(barrier, inc=1, device_id=device, device_id_type=MESH)

    copies = []
    used_sems = 0
    for (dx, dy), kind, moves in links:
        device = (gx + dx, gy + dy, 1 if kind == 1 else gz)
        group_of = []
        for a, b in moves:
            group_of.append(
                pltpu.make_async_remote_copy(
                    src_ref=a, dst_ref=b, send_sem=send_sem.at[used_sems],
                    recv_sem=recv_sem.at[used_sems], device_id=device, device_id_type=MESH,
                )
            )
            used_sems += 1
        copies.append(group_of)

    def wait_if(link, k):
        @pl.when(gets_if(link))
        def _():
            for copy in copies[k]:
                copy.wait_recv()

    def relay():
        wait_if(cut, links.index(cut))
        for link, pair in zip(links, copies):
            if link[1] == 2:

                @pl.when(sends_if(link))
                def _(pair=pair):
                    for copy in pair:
                        copy.start()

    def first_sends():
        pl.semaphore_wait(barrier, targets + 10)
        for link, pair in zip(links, copies):
            if link[1] == 0:

                @pl.when(sends_if(link))
                def _(pair=pair):
                    pair[1].start()

    first_sends()
    kappa, rho = (
        jnp.concatenate([mat_ref[j, :, y, :] for y in range(ny)], axis=1) for j in range(2)
    )
    at_low = gz == 1
    cell = lax.broadcasted_iota(jnp.int32, (n, 128), 0)
    lane = lax.broadcasted_iota(jnp.int32, (n, 128), 1)
    edge_z = jnp.where(at_low, 0, nz - 1)
    hot = jnp.logical_and(cell == lane * nz + edge_z, lane < ny).astype(F32).astype(BF16)
    width = nx * nz
    for j, rows in enumerate((kappa, rho)):
        faces_ref[j : j + 1, :] = jnp.concatenate(
            [rows[x : x + 1, (ny - 1) * nz :] for x in range(nx)], axis=1
        )
        faces_ref[4 + j : 5 + j, :] = jnp.concatenate(
            [rows[x : x + 1, :nz] for x in range(nx)], axis=1
        )
        faces_ref[2 + j : 3 + j, :] = jnp.concatenate(
            [rows[nx - 1 :], jnp.zeros((1, width - n), F32)], axis=1
        )
        edge_rows = exact(rows, hot)
        turned = jnp.concatenate([edge_rows, jnp.zeros((128 - nx, 128), F32)], axis=0).T
        fz_ref[j : j + 1, :] = jnp.concatenate(
            [turned[y : y + 1, :nx] for y in range(ny)]
            + [edge_rows[:1, :nx], edge_rows[nx - 1 :, :nx]]
            + [jnp.zeros((1, 256 - (ny + 2) * nx), F32)],
            axis=1,
        )

    faces_ref[6:, :] = jnp.zeros((2, width), F32)
    fz_ref[2:, :] = jnp.zeros((6, 256), F32)

    def z_edge(x, y, count):
        tall, low = vbuf[x, y, nz - 16 :, :], vbuf[x, y, :16, :]
        picked = jnp.where(at_low, low.astype(F32)[:, 0, :], tall.astype(F32)[:, 15, :])
        return picked.astype(BF16)

    def later_sends():
        for load in loads[5:]:
            load.wait()
        for y in range(ny):
            zf_ref[y] = z_edge(slice(None), y, nx)
        zx_ref[...] = jnp.zeros_like(zx_ref)
        for j, x in enumerate((0, nx - 1)):
            zx_ref[j, :ny] = z_edge(x, slice(None), ny)
        for link, pair in zip(links, copies):

            if link[1] < 2:

                @pl.when(sends_if(link))
                def _(link=link, pair=pair):
                    for copy in pair if link[1] else pair[:1]:
                        copy.start()

    weights[0].wait()
    starts = np.cumsum([0] + [hi - lo for lo, hi in WINDOWS])
    zero = jnp.zeros((1, n), F32)
    filtered = jnp.concatenate(
        [
            exact(kappa[:, lo:hi], wp_ref[starts[t] : starts[t + 1], :128])
            for t, (lo, hi) in enumerate(WINDOWS)
        ],
        axis=1,
    )
    around = (
        jnp.concatenate([zero, filtered[:-1]], axis=0)
        + 2.0 * filtered
        + jnp.concatenate([filtered[1:], zero], axis=0)
    )
    diag = 0.5 * (3.5 * kappa + PC * around - 0.5 * kappa)
    coef_v = diag + 0.5 * kappa
    coef_s = PC * kappa
    coef_m = PM * rho

    def load_plane(x):
        if x < nx:
            if x < 5:
                loads[x].wait()
            vt[x // 2, :, (x % 2) * n : (x % 2 + 1) * n] = vbuf[x].reshape(n, cols).T

    def stage_a(x):
        if x < nx:
            load_plane(x)
            for t, (lo, hi) in enumerate(WINDOWS):
                base = (x % 2) * n
                fbuf[x % 6, :, t * 256 : (t + 1) * 256] = nn(
                    vt[x // 2, :, base + lo : base + hi], wp_ref[starts[t] : starts[t + 1]]
                )

    chunk = 32

    def stage_b(x, lo, hi):
        half = (x % 2) * n
        buf = (x // 2) % 2
        for r in range(lo, hi, chunk):
            rows = slice(r, r + chunk)
            for t in range(n // 128):
                cv, cs, cm = (
                    c[x : x + 1, t * 128 : (t + 1) * 128] for c in (coef_v, coef_s, coef_m)
                )
                at_s = slice(t * 256, t * 256 + 128)
                at_m = slice(t * 256 + 128, (t + 1) * 256)
                at_v = slice(half + t * 128, half + (t + 1) * 128)
                s = 2.0 * fbuf[x % 6, rows, at_s]
                m = 4.0 * fbuf[x % 6, rows, at_m]
                for near in (x - 1, x + 1):
                    if 0 <= near < nx:
                        s = s + fbuf[near % 6, rows, at_s]
                        m = m + fbuf[near % 6, rows, at_m]
                v = vt[x // 2, rows, at_v].astype(F32)
                ys[x // 2, rows, at_v] = (cv * v - cs * s).astype(BF16)
                ym[buf, rows, at_v] = (cm * m).astype(BF16)

    def stage_c(pair):
        if pair < 0:
            return
        part = nt(vt[pair], ym[pair % 2])
        if pair == 0:
            acc[1] = part
        else:
            acc[1] += part

    pairs = nx // 2
    for x in range(3):
        stage_a(x)
    for i in range(pairs):
        for x in range(2):
            stage_a(2 * i + 3 + x)
            stage_b(2 * i + x, 0, cols)
        stage_c(i - 1)
        if i == 0:
            later_sends()
        if i == RELAY:
            relay()
    stage_c(pairs - 1)
    for load in weights[1:]:
        load.wait()

    def wait_for(*ks):
        for k in ks:
            wait_if(links[k], k)

    def row(k, r, lo, hi):
        return fh[k, r : r + 1, lo:hi]

    def wide(x):
        return jnp.concatenate(x, axis=1)

    used = (hx_n + 2) * nz
    blank = jnp.zeros((1, 16), F32)
    edge = (nx - 1) * nz

    later = []

    def group(k_at, m_at, halo, kh, rh, own, ko, ro, w_ref, windows):
        k, m = halo.shape[0], own.shape[1]
        ht[:, k_at : k_at + k] = halo.T
        owned[:, m_at : m_at + m] = own
        rc = jnp.broadcast_to(rh, (128, k)).T
        spans = np.cumsum([0] + [hi - lo for lo, hi in windows])
        for t, (lo, hi) in enumerate(windows):
            lanes = slice(t * 128, (t + 1) * 128)
            wm = w_ref[spans[t] : spans[t + 1], 128:].astype(F32)
            lm = (wm * (PM * (rc[lo:hi] + ro[:, lanes]))).astype(BF16)
            at = slice(m_at + t * 128, m_at + (t + 1) * 128)
            um[:, at] = nn(ht[:, k_at + lo : k_at + hi], lm).astype(BF16)

        def stiff():
            kc = jnp.broadcast_to(kh, (128, k)).T
            far = jnp.zeros((1, k), F32)
            for t, (lo, hi) in enumerate(windows):
                lanes = slice(t * 128, (t + 1) * 128)
                tile = w_ref[spans[t] : spans[t + 1], :128]
                wc = tile.astype(F32)
                ls = (wc * ((-PC) * (kc[lo:hi] + ko[:, lanes]))).astype(BF16)
                fbuf[t, :, :128] = nn(ht[:, k_at + lo : k_at + hi], ls)
                own_diag = (0.5 * PC) * jnp.sum(wc * kc[lo:hi], axis=0, keepdims=True)
                part = (0.5 * PC) * exact_nt(ko[:, lanes], tile)
                sides = [jnp.zeros((1, lo), F32), part, jnp.zeros((1, k - hi), F32)]
                far = far + wide([x for x in sides if x.shape[1]])
                at = slice(m_at + t * 128, m_at + (t + 1) * 128)
                for r in range(0, cols, 64):
                    rows = slice(r, r + 64)
                    us[rows, at] = (
                        own_diag * owned[rows, at].astype(F32) + fbuf[t, rows, :128]
                    ).astype(BF16)
            for r in range(0, cols, 32):
                rows = slice(r, r + 32)
                at = slice(k_at, k_at + k)
                hfar[rows, at] = (far * ht[rows, at].astype(F32)).astype(BF16)

        later.append(stiff)

    ky = 2 * 16 + used
    acc[0] = nt(vt[0], ys[0])
    for pair in range(1, EARLY):
        acc[0] += nt(vt[pair], ys[pair])
    wait_for(3)
    group(
        2 * ky, 2 * n, hx[...].reshape(n, cols), row(3, 2, 0, n), row(3, 3, 0, n),
        vt[0, :, :n], kappa[:1], rho[:1], wp_ref, WINDOWS,
    )

    wait_for(*range(6, 14))
    nf = nx * ny
    low, high = (nf - nx, nf), (0, nx)

    def zpick(r):
        spans = [(0, nf), low, high, (nf + nx, nf + 2 * nx), (nf, nf + nx), low, high, low, high]
        return wide([fhz[k, r : r + 1, lo:hi] for k, (lo, hi) in enumerate(spans)])

    group(
        2 * ky + n, 3 * n, hz[...].reshape((ny + 8) * nx, cols), zpick(0), zpick(1),
        zf_ref[...].reshape(nf, cols).T, fz_ref[:1, :nf], fz_ref[1:2, :nf],
        wz_ref, ZWINDOWS,
    )

    wait_for(0, 1)
    none = jnp.zeros((16, cols), BF16)
    lower = lambda r: wide([blank, row(1, r, edge, edge + nz), row(0, r, 0, used - nz), blank])
    group(
        0, 0, jnp.concatenate([none, hy[...].reshape(used, cols), none], axis=0),
        lower(0), lower(1), vbuf[:hx_n, 0].reshape(hx_n * nz, cols).T,
        *(wide([rows[x : x + 1, :nz] for x in range(hx_n)]) for rows in (kappa, rho)),
        wy_ref, YWINDOWS,
    )
    wait_for(2, 4)
    upper = lambda r: wide(
        [blank, faces_ref[r : r + 1, (hx_n - 1) * nz :], row(2, r, 0, nz), blank]
    )
    mine = vbuf[hx_n - 1 :, ny - 1].reshape(used - nz, cols)
    group(
        ky, n, jnp.concatenate([none, mine, hc[...], none], axis=0),
        upper(0), upper(1), hu[...].reshape(hx_n * nz, cols).T,
        row(4, 4, hx_n * nz, nx * nz), row(4, 5, hx_n * nz, nx * nz), wy_ref, YWINDOWS,
    )

    core, zl = lax.rem(gx, 2), gx // 2
    place = {"x": gy // 4, "y": lax.rem(gy, 4), "z": gz * 2 + zl}

    def device_of(dim, at):
        x, y, z = (at if dim == d else place[d] for d in "xyz")
        return (lax.rem(z, 2) * 2 + core, x * 4 + y, z // 2)

    pending = []

    def send(source, target, sem, device):
        copy = pltpu.make_async_remote_copy(
            src_ref=source, dst_ref=target, send_sem=rsend.at[sem], recv_sem=rrecv.at[sem],
            device_id=device, device_id_type=MESH,
        )
        copy.start()
        pending.append(copy)
        return copy

    def pick_part(buf, dims, dim, at):
        index = []
        for d in dims:
            hit = {"l": lax.rem(at, 2), "h": at // 2}.get(d) if dim == "z" else at if d == dim else None
            index.append(slice(None) if hit is None else hit)
        return tuple(index)

    half = cols // 2
    low_rows = lax.broadcasted_iota(jnp.int32, (16, 8, half), 1) < 4

    def symmetrize(h):
        for b in range(4):
            block = slice(b * 128, (b + 1) * 128)
            total = (acc[h, block] + acc[h, :, block].T) * scale
            left, right = total[:, :half].reshape(16, 8, half), total[:, half:].reshape(16, 8, half)
            first = jnp.where(low_rows, left, pltpu.roll(right, 4, 1))
            second = jnp.where(low_rows, pltpu.roll(left, 4, 1), right)
            q[h, b // 2, b % 2, :, :, 0] = first.reshape(4, 4, 8, half)
            q[h, b // 2, b % 2, :, :, 1] = second.reshape(4, 4, 8, half)

    matrix = (1, 1, 0, 0)
    held = [None] * tiles

    def swap(t):
        lanes = slice((t % 2) * 128, (t % 2 + 1) * 128)
        held[t] = send(
            q.at[matrix[t], :, 1 - core, :, :, :, :, lanes], stage[0][t], t,
            (zl * 2 + 1 - core, gy, gz),
        )

    def swapped(t):
        lanes = slice((t % 2) * 128, (t % 2 + 1) * 128)
        held[t].wait_recv()
        stage[0][t][...] += q[matrix[t], :, core, :, :, :, :, lanes]
        buf = (stage[0][t], "lxyh")
        held[t] = (buf, exchange_start(t, 0, buf, pick_part, place, device_of, send, stage))

    def advance(t, s):
        (buf, dims), copies_t = held[t]
        dim = ORDERS[t][s]
        total = buf[pick_part(buf, dims, dim, place[dim])]
        for j, copy in enumerate(copies_t):
            copy.wait_recv()
            total = total + stage[s + 1][t][j]
        if s == 2:
            rows = slice(4 * matrix[t], 4 * matrix[t] + 4)
            out_ref[rows, (t % 2) * 128 : (t % 2 + 1) * 128] = total[:4]
            out_ref[rows, half + (t % 2) * 128 : half + (t % 2 + 1) * 128] = total[4:]
            return
        kept = keep[s][t]
        kept[...] = total
        buf = (kept, "".join(d for d in dims if d not in GONE[dim]))
        held[t] = (buf, exchange_start(t, s + 1, buf, pick_part, place, device_of, send, stage))

    acc[1] += nt(owned[...], um[...])
    symmetrize(1)
    swap(0)
    swap(1)
    for stiff in later:
        stiff()
    acc[0] += nt(owned[...], us[...])
    acc[0] += nt(ht[...], hfar[...])
    for pair in range(EARLY, pairs):
        acc[0] += nt(vt[pair], ys[pair])
        if pair == 6:
            swapped(0)
            swapped(1)
    symmetrize(0)
    swap(2)
    swap(3)
    swapped(2)
    swapped(3)
    for s in range(3):
        for t in range(tiles):
            advance(t, s)
    for copy in pending:
        copy.wait_send()
    for k, link in enumerate(links):
        @pl.when(sends_if(link))
        def _(k=k):
            for copy in copies[k]:
                copy.wait_send()


def local_sums(eigvecs, material):
    nx, ny, nz, cols = eigvecs.shape
    n = ny * nz
    count = {a: lax.axis_size(a) for a in ("gx", "gy", "gz")}
    cells = nx * ny * nz * count["gx"] * count["gy"] * count["gz"]
    plane, wy, wz = (jnp.asarray(w, BF16) for w in weight_arrays(nx, ny, nz))
    width = nx * nz
    shapes, keeps = stage_shapes()
    own_cells = 3 * n + nx * ny
    halo_cells = 2 * (32 + (nx // 2 + 2) * nz) + n + (ny + 8) * nx
    anyspace = pl.BlockSpec(memory_space=pl.ANY)
    vmem = pl.BlockSpec(memory_space=pltpu.VMEM)
    kernel = lambda *refs: local_kernel(
        (nx, ny, nz, cols, count["gx"], count["gy"]), 0.5 / cells, *refs
    )
    return pl.pallas_call(
        kernel,
        out_shape=pltpu.VMEM((8, cols), F32),
        in_specs=[anyspace, vmem] + [anyspace] * 3,
        out_specs=vmem,
        scratch_shapes=[
            pltpu.VMEM((nx, ny, nz, cols), BF16),
            pltpu.VMEM((nx // 2, cols, 2 * n), BF16),
            pltpu.VMEM((6, cols, 2 * n), F32),
            pltpu.VMEM((2, cols, 2 * n), BF16),
            pltpu.VMEM((2, cols, cols), F32),
            pltpu.VMEM((nx // 2 + 2, nz, cols), BF16),
            pltpu.VMEM((ny, nz, cols), BF16),
            pltpu.VMEM((ny + 8, nx, cols), BF16),
            pltpu.VMEM((5, 8, width), F32),
            pltpu.SemaphoreType.DMA((nx,)),
            pltpu.SemaphoreType.DMA((29,)),
            pltpu.SemaphoreType.DMA((29,)),
            pltpu.VMEM((2, 2, 2, 4, 4, 2, 8, cols // 2), F32),
            pltpu.SemaphoreType.DMA((10 * tiles,)),
            pltpu.SemaphoreType.DMA((10 * tiles,)),
            pltpu.VMEM((8, width), F32),
            pltpu.VMEM((ny, nx, cols), BF16),
            pltpu.VMEM((2, nx, cols), BF16),
            pltpu.VMEM(plane.shape, BF16),
            pltpu.VMEM(wy.shape, BF16),
            pltpu.VMEM(wz.shape, BF16),
            pltpu.SemaphoreType.DMA((3,)),
            pltpu.VMEM((nx // 2, cols, 2 * n), BF16),
            pltpu.VMEM((cols, halo_cells), BF16),
            pltpu.VMEM((cols, halo_cells), BF16),
        ]
        + [pltpu.VMEM((cols, own_cells), BF16)] * 3
        + [pltpu.VMEM((nx // 2, nz, cols), BF16), pltpu.VMEM((nz, cols), BF16)]
        + [pltpu.VMEM((2, nx, cols), BF16), pltpu.VMEM((8, 256), F32), pltpu.VMEM((9, 8, 256), F32)]
        + [pltpu.VMEM(x, F32) for row in shapes + keeps for x in row],
        compiler_params=pltpu.CompilerParams(
            collective_id=0, has_side_effects=True, vmem_limit_bytes=63 * 1024 * 1024
        ),
        name="local_sums",
    )(eigvecs, material, plane, wy, wz)


def per_device(eigvecs, material):
    both = local_sums(eigvecs, material)
    return both[:4], both[4:]


def solution(mesh):
    return jax.shard_map(
        per_device,
        mesh=mesh,
        in_specs=(P("gx", "gy", "gz", None), P(None, "gx", "gy", "gz")),
        out_specs=(P(("gx", "gy", "gz"), None), P(("gx", "gy", "gz"), None)),
        check_vma=False,
    )
```
